512 devices in a mesh: dp: 32 (over z, x), tensor: 16 (over y, core).
Axes of the slice: x: 4, y: 8, z: 8, core: 2. Of those that a mesh axis runs over, the one named last changes fastest.
Arguments:
- tokens: bfloat16 [4096, 4096], P('dp', 'tensor'), may hold values from -6 to 6
- out_grad: bfloat16 [4096, 4096], P('dp', 'tensor'), may hold values from -6 to 6
- up_weight: bfloat16 [4096, 14336], P('dp', 'tensor'), may hold values from -0.09375 to 0.09375
- down_weight: bfloat16 [14336, 4096], P('tensor', 'dp'), may hold values from -0.046875 to 0.046875
- up_accum: float32 [32, 256, 14336], P('dp', None, 'tensor'), may hold values from -6 to 6
- down_accum: float32 [32, 14336, 256], P('dp', 'tensor'), may hold values from -6 to 6
- up_q: float32 [14336, 32], P('tensor'), may hold values from -6 to 6
- down_q: float32 [256, 32], replicated, may hold values from -6 to 6
Outputs:
- input_grad: bfloat16 [4096, 4096], P('dp', 'tensor')
- up_error: float32 [32, 256, 14336], P('dp', None, 'tensor')
- up_left: float32 [256, 32], replicated
- up_right: float32 [14336, 32], P('tensor')
- down_error: float32 [32, 14336, 256], P('dp', 'tensor')
- down_left: float32 [14336, 32], P('tensor')
- down_right: float32 [256, 32], replicated
The draws below stay inside these ranges and needn't reach their ends.
All inputs are finite; a program needn't handle non-finite values.
Results may differ from the reference program's by a relative error of at most 0.02.
Values may be sent and summed in bfloat16 or wider, within the bound.
A program may use at most 128 MiB of HBM per device.

```python
import math
import jax
import jax.numpy as jnp
from jax import lax

D = 4096
FF_DEV = 896
TOK = 128
WIN = 256
RANK = 32
FF = 14336
TOKENS = 4096
N_DP = 32
N_TENSOR = 16


def shard_levels(rng, shape, shards, low, top_value):
    factor_of = 1.0
    for position, blocks in shards:
        heights = jax.random.uniform(jax.random.fold_in(jax.random.fold_in(rng, 6), position), (blocks,), jnp.float32, low / len(shards), top_value / len(shards))
        factor_of = factor_of * jnp.repeat(jnp.exp(heights), shape[position] // blocks).reshape((-1,) + (1,) * (len(shape) - 1 - position))
    return factor_of


def gaussian(rng, dims, deviation, limit, pieces=(), held_as=jnp.bfloat16):
    loudness = shard_levels(rng, dims, pieces, -0.22, 0.18) if pieces else 1.0
    result = jax.random.normal(rng, dims, jnp.float32) * deviation * loudness
    return jnp.minimum(jnp.maximum(result, -limit), limit).astype(held_as)


def setup_inputs(seed: int = 0) -> dict:
    arg_keys = jax.random.split(jax.random.key(seed), 9)
    tokens = gaussian(arg_keys[0], (TOKENS, D), 1.0, 6.0, ((0, 32), (1, 16)))
    out_grad = gaussian(arg_keys[1], (TOKENS, D), 1.0, 6.0, ((0, 32), (1, 16)))
    up_weight = gaussian(arg_keys[2], (D, FF), D ** -0.5, 0.09375, ((0, 32), (1, 16)))
    down_weight = gaussian(arg_keys[3], (FF, D), FF ** -0.5, 0.046875, ((0, 16), (1, 32)))
    up_accum = gaussian(arg_keys[4], (N_DP, WIN, FF), 1.0, 6.0, ((0, 32), (2, 16)), jnp.float32)
    down_accum = gaussian(arg_keys[5], (N_DP, FF, WIN), 1.0, 6.0, ((0, 32), (1, 16)), jnp.float32)
    up_q = gaussian(arg_keys[6], (FF, RANK), 1.0, 6.0, ((0, 16),), jnp.float32)
    down_q = gaussian(arg_keys[7], (WIN, RANK), 1.0, 6.0, (), jnp.float32)
    return dict(tokens=tokens, out_grad=out_grad, up_weight=up_weight, down_weight=down_weight, up_accum=up_accum, down_accum=down_accum, up_q=up_q, down_q=down_q)


def orthonormal(left_sum):
    gram = jnp.dot(left_sum.T, left_sum, precision=lax.Precision.HIGHEST)
    lower_factor = jnp.linalg.cholesky(gram)
    return lax.linalg.triangular_solve(lower_factor, left_sum, left_side=False, lower=True, transpose_a=True)

def compress(matrix, start_q):
    left_sum = jnp.einsum('rab,bk->ak', matrix, start_q, precision=lax.Precision.HIGHEST)
    left = orthonormal(left_sum)
    right = jnp.einsum('rab,ak->bk', matrix, left, precision=lax.Precision.HIGHEST) / N_DP
    approx = jnp.dot(left, right.T, precision=lax.Precision.HIGHEST)
    return (matrix - approx[None], left, right)

def reference(tokens, out_grad, up_weight, down_weight, up_accum, down_accum, up_q, down_q):
    preact = jnp.dot(tokens.astype(jnp.float32), up_weight.astype(jnp.float32), preferred_element_type=jnp.float32)
    back_act = jnp.dot(out_grad.astype(jnp.float32), down_weight.T.astype(jnp.float32), preferred_element_type=jnp.float32)
    squash = jax.nn.sigmoid(preact)
    act_out = (preact * squash).astype(jnp.bfloat16)
    hidden_grad = (back_act * squash * (1.0 + preact * (1.0 - squash))).astype(jnp.bfloat16)
    grad_blocks = hidden_grad.reshape(TOKENS, N_TENSOR, FF_DEV).transpose(1, 0, 2)
    weight_blocks = up_weight.reshape(D, N_TENSOR, FF_DEV).transpose(1, 0, 2)

    def add_block(running, blocks):
        partial_sum = jnp.dot(blocks[0].astype(jnp.float32), blocks[1].T.astype(jnp.float32), preferred_element_type=jnp.float32)
        rounded = lax.optimization_barrier(partial_sum.astype(jnp.bfloat16))
        return (running + rounded.astype(jnp.float32), 0)
    running, unused = lax.scan(add_block, jnp.zeros((TOKENS, D), jnp.float32), (grad_blocks, weight_blocks))
    input_grad = running.astype(jnp.bfloat16)
    grad_scale = 1.0 / math.sqrt(TOK)
    token_window = tokens.reshape(N_DP, TOK, D)[:, :, :WIN].astype(jnp.float32)
    grad_window = out_grad.reshape(N_DP, TOK, D)[:, :, :WIN].astype(jnp.float32)
    hidden_rep = hidden_grad.reshape(N_DP, TOK, FF).astype(jnp.float32)
    act_rep = act_out.reshape(N_DP, TOK, FF).astype(jnp.float32)
    up_matrix = up_accum + jnp.einsum('rtw,rtf->rwf', token_window, hidden_rep, precision=lax.Precision.HIGHEST) * grad_scale
    down_matrix = down_accum + jnp.einsum('rtf,rtw->rfw', act_rep, grad_window, precision=lax.Precision.HIGHEST) * grad_scale
    up_error, up_left, up_right = compress(up_matrix, up_q)
    down_error, down_left, down_right = compress(down_matrix, down_q)
    return (input_grad, up_error, up_left, up_right, down_error, down_left, down_right)
```

```python
import functools
import math

import jax
import jax.numpy as jnp
from jax import lax
from jax.experimental import pallas as pl
from jax.experimental.pallas import tpu as pltpu
from jax.sharding import PartitionSpec as P

MESH = pl.DeviceIdType.MESH
HI = lax.Precision.HIGHEST
NZ, NX, NY = 8, 4, 8
NDP, NT = 32, 16
F32, BF16 = jnp.float32, jnp.bfloat16


def wrap(a, n):
    return lax.rem(a + 4 * n, n)


def dot_nt(a, b, precision=None):
    return lax.dot_general(
        a, b, (((1,), (1,)), ((), ())), preferred_element_type=F32, precision=precision
    )


def dot_nn(a, b, precision=None):
    return jnp.dot(a, b, preferred_element_type=F32, precision=precision)


def inverse_factor(gram):
    n = gram.shape[0]
    rows = lax.broadcasted_iota(jnp.int32, (n, 128), 0)
    lanes = lax.broadcasted_iota(jnp.int32, (n, 128), 1)
    unit = jnp.where(lanes == rows + n, 1.0, 0.0).astype(F32)
    work = jnp.concatenate([gram, jnp.zeros((n, 128 - n), F32)], axis=1) + unit
    for k in range(n):
        scale = lax.rsqrt(work[k : k + 1, k : k + 1])
        line = work[k : k + 1, :] * scale
        col = work[:, k : k + 1] * scale
        work = jnp.where(rows > k, work - col * line, jnp.where(rows == k, line, work))
    return work[:, n : 2 * n]


def kernel(
    tok, og, wu, wd, uq, dq, uacc, dacc,
    ig_out, ul_out, ur_out, dl_out, dr_out, uerr, derr,
    A, WU, WD, WIN, PF, SB, FB, RB, HG, IGP, IGX, PS, RY, FY, IGO, MU, MD,
    P28, R28, L28, P8, R8T, R8D, L8, GR,
    acc_sem, err_sem, ring_s, ring_r, xs, xr, ys, yr, ds, dr, ws, wr,
    rs_s, rs_r, hs, hr, ps_s, ps_r, ry_s, ry_r, fs, fr, cs, cr, gs, gr,
):
    dp, t = lax.axis_index("dp"), lax.axis_index("tensor")
    z, x = dp // NX, lax.rem(dp, NX)
    y, c = t // 2, lax.rem(t, 2)
    mine = x // 2 == c
    xl, xrr = wrap(x - 1, NX), wrap(x + 1, NX)
    sib = (dp, t + 1 - 2 * c)
    tokens = tok.shape[0]
    grad_scale = 1.0 / math.sqrt(tokens)

    def lanes_of(i):
        return pl.ds(pl.multiple_of(i * 128, 128), 128)

    def rcopy(src, dst, s, r, dev):
        return pltpu.make_async_remote_copy(
            src_ref=src, dst_ref=dst, send_sem=s, recv_sem=r, device_id=dev, device_id_type=MESH
        )

    def drain(ref, sem):
        pltpu.make_async_copy(ref, ref, sem).wait()

    def at_x(xi):
        return (z * NX + xi, t)

    load_u = pltpu.make_async_copy(uacc.at[0], MU, acc_sem.at[0])
    load_d = pltpu.make_async_copy(dacc.at[0], MD, acc_sem.at[1])
    load_u.start()
    load_d.start()

    WU[z] = wu[...]
    WD[:, lanes_of(z)] = wd[...]
    for h in range(2):

        @pl.when(jnp.logical_and(mine, lax.rem(x, 2) == h))
        def _():
            A[0, x, :, lanes_of(y)] = tok[:, h * 128 : (h + 1) * 128]
            A[1, x, :, lanes_of(y)] = og[:, h * 128 : (h + 1) * 128]

    @pl.when(t == 0)
    def _():
        WIN[0] = tok[...]
        WIN[1] = og[...]

    barrier = pltpu.get_barrier_semaphore()

    def greet_dp(j, carry):
        @pl.when(j != dp)
        def _():
            pl.semaphore_signal(barrier, inc=1, device_id=(j, t), device_id_type=MESH)

        return carry

    def greet_t(j, carry):
        @pl.when(j != t)
        def _():
            pl.semaphore_signal(barrier, inc=1, device_id=(dp, j), device_id_type=MESH)

        return carry

    lax.fori_loop(0, NDP, greet_dp, 0)
    lax.fori_loop(0, NT, greet_t, 0)

    @pl.when(jnp.logical_not(mine))
    def _():
        for h in range(2):
            pl.semaphore_signal(
                barrier,
                inc=1,
                device_id=(z * NX + 2 * c + h, 2 * y + x // 2),
                device_id_type=MESH,
            )

    pl.semaphore_wait(barrier, NDP + NT - 2 + 2 * jnp.where(mine, 0, 1).astype(jnp.int32))

    def slot(mat, zi, half):
        if mat == 0:
            return WU.at[zi, pl.ds(half * 64, 64)]
        return WD.at[pl.ds(half * 448, 448), lanes_of(zi)]

    def ring(mat, way, step, half):
        if way == 0:
            zi, to = wrap(z - step + 1, NZ), wrap(z + 1, NZ)
        else:
            zi, to = wrap(z + step - 1, NZ), wrap(z - 1, NZ)
        src = slot(mat, zi, half)
        if step == 1:
            src = wu.at[pl.ds(half * 64, 64)] if mat == 0 else wd.at[pl.ds(half * 448, 448)]
        i = (mat, way, half, step - 1)
        return rcopy(src, slot(mat, zi, half), ring_s.at[i], ring_r.at[i], (to * NX + x, t))

    def ring_arrived(mat, way, step, half):
        zi = wrap(z - step, NZ) if way == 0 else wrap(z + step, NZ)
        ref = slot(mat, zi, half)
        i = (mat, way, half, step - 1)
        rcopy(ref, ref, ring_s.at[i], ring_r.at[i], (dp, t)).wait_recv()

    def ring_parts(step):
        if step < 4:
            return [(way, half) for half in range(2) for way in range(2)]
        return [(0, 0), (1, 1)]

    def ring_send(mat, step, halves=(0, 1)):
        for way, half in ring_parts(step):
            if half in halves:
                ring(mat, way, step, half).start()

    def ring_pass(mat, step):
        nxt = ring_parts(step)
        for way, half in ring_parts(step - 1):
            ring_arrived(mat, way, step - 1, half)
            if (way, half) in nxt:
                ring(mat, way, step, half).start()

    def ring_end(mat):
        for way, half in ring_parts(4):
            ring_arrived(mat, way, 4, half)

    ring_send(0, 1)

    def piece(arr, h):
        xd = 2 * c + h
        src = (tok, og)[arr].at[:, pl.ds(h * 128, 128)]
        return rcopy(
            src,
            A.at[arr, x, :, lanes_of(y)],
            xs.at[arr, h],
            xr.at[arr, lax.rem(x, 2)],
            (z * NX + xd, 2 * y + x // 2),
        )

    def foreign(h):
        return jnp.logical_not(jnp.logical_and(mine, lax.rem(x, 2) == h))

    for arr in range(2):
        for h in range(2):

            @pl.when(foreign(h))
            def _():
                piece(arr, h).start()

    def pair(arr, yi):
        return A.at[arr, pl.ds(2 * c, 2), :, lanes_of(yi)]

    def spread(arr, off):
        yd = wrap(y + off, NY)
        return rcopy(pair(arr, y), pair(arr, y), ys.at[arr, off], yr.at[arr, off], (dp, 2 * yd + c))

    def to_sibling(arr, yi, off):
        return rcopy(pair(arr, yi), pair(arr, yi), ds.at[arr, off], dr.at[arr, off], sib)

    ring_send(1, 1, (0,))
    for arr in range(2):
        for h in range(2):

            @pl.when(foreign(h))
            def _():
                ref = A.at[arr, 2 * c + h, :, lanes_of(y)]
                rcopy(ref, ref, xs.at[arr, h], xr.at[arr, h], (dp, t)).wait_recv()

        for off in (4, 3, 5, 2, 6, 1, 7):
            spread(arr, off).start()
        to_sibling(arr, y, 0).start()

    @pl.when(t == 0)
    def _():
        def one(j, carry):
            rcopy(tok, WIN.at[0], ws.at[0], wr.at[0], (dp, j)).start()
            rcopy(og, WIN.at[1], ws.at[1], wr.at[1], (dp, j)).start()
            return carry

        lax.fori_loop(1, NT, one, 0)

    def y_arrivals(arr):
        for off in (1, 7, 2, 6, 3, 5, 4):
            yi = wrap(y - off, NY)
            ref = pair(arr, yi)
            rcopy(ref, ref, ys.at[arr, off], yr.at[arr, off], (dp, t)).wait_recv()
            to_sibling(arr, yi, off).start()

    def sibling_arrivals(arr):
        for off in range(NY):
            yi = wrap(y - off, NY)
            ref = A.at[arr, pl.ds(2 - 2 * c, 2), :, lanes_of(yi)]
            rcopy(ref, ref, ds.at[arr, off], dr.at[arr, off], (dp, t)).wait_recv()

    ring_pass(0, 2)
    ring_send(1, 1, (1,))
    ring_pass(0, 3)
    ring_pass(1, 2)
    ring_pass(0, 4)
    y_arrivals(0)
    ring_pass(1, 3)
    sibling_arrivals(0)
    ring_end(0)

    def products(mat):
        def one(d, carry):
            xi = wrap(x + d, NX)
            if mat == 0:
                PF[0, d] = dot_nn(A[0, xi], WU[...].reshape(NZ * 128, WU.shape[2]))
            else:
                PF[1, d] = dot_nt(A[1, xi], WD[...])
            return carry

        lax.fori_loop(0, NX, one, 0)

    half_rows = tokens // 2
    top, bot = pl.ds(0, half_rows), pl.ds(half_rows, half_rows)

    def rs_copy(mat, i):
        src = (SB.at[mat, 1, top], SB.at[mat, 1, bot], SB.at[mat, 0, bot],
               SB.at[mat, 2, top], SB.at[mat, 0, top], SB.at[mat, 2, bot])[i]
        dst = (FB.at[mat, 0], FB.at[mat, 1], RB.at[mat, 0, bot],
               RB.at[mat, 1, top], RB.at[mat, 0, top], RB.at[mat, 1, bot])[i]
        to = at_x(xrr if i % 2 == 0 else xl)
        return rcopy(src, dst, rs_s.at[mat, i], rs_r.at[mat, i], to)

    def rs_first(mat):
        SB[mat, 1] = PF[mat, 2].astype(BF16)
        rs_copy(mat, 0).start()
        rs_copy(mat, 1).start()
        SB[mat, 0, half_rows:] = PF[mat, 1, half_rows:].astype(BF16)
        rs_copy(mat, 2).start()
        SB[mat, 2, :half_rows] = PF[mat, 3, :half_rows].astype(BF16)
        rs_copy(mat, 3).start()

    def rs_second(mat):
        rs_copy(mat, 0).wait_recv()
        SB[mat, 0, :half_rows] = (PF[mat, 1, :half_rows] + FB[mat, 0].astype(F32)).astype(BF16)
        rs_copy(mat, 4).start()
        rs_copy(mat, 1).wait_recv()
        SB[mat, 2, half_rows:] = (PF[mat, 3, half_rows:] + FB[mat, 1].astype(F32)).astype(BF16)
        rs_copy(mat, 5).start()

    def rs_end(mat):
        for i in range(2, 6):
            rs_copy(mat, i).wait_recv()

    products(0)
    rs_first(0)
    y_arrivals(1)
    ring_pass(1, 4)
    rs_second(0)
    sibling_arrivals(1)
    ring_end(1)
    products(1)
    rs_first(1)
    rs_end(0)
    load_u.wait()
    load_d.wait()

    @pl.when(t != 0)
    def _():
        for arr in range(2):
            rcopy(WIN.at[arr], WIN.at[arr], ws.at[arr], wr.at[arr], (dp, t)).wait_recv()

    rs_second(1)
    rs_end(1)
    preact = PF[0, 0] + RB[0, 0].astype(F32) + RB[0, 1].astype(F32)
    back = PF[1, 0] + RB[1, 0].astype(F32) + RB[1, 1].astype(F32)
    squash = jax.nn.sigmoid(preact)
    act = (preact * squash).astype(BF16)
    hidden = (back * squash * (1.0 + preact * (1.0 - squash))).astype(BF16)
    HG[x] = hidden

    MU[...] += dot_nn(WIN[0].T, hidden) * grad_scale
    MD[...] += dot_nn(act.T, WIN[1]) * grad_scale

    def put28(k, arr):
        for g in range(4):
            for l in range(7):
                P28[k, g * 7 + l] = arr[8 * g : 8 * g + 8, 128 * l : 128 * l + 128]

    def put8(k, arr):
        for g in range(4):
            for l in range(2):
                P8[k, g * 2 + l] = arr[8 * g : 8 * g + 8, 128 * l : 128 * l + 128]

    def get(buf, k, n):
        return jnp.concatenate(
            [jnp.concatenate([buf[k, g * n + l] for l in range(n)], axis=1) for g in range(4)],
            axis=0,
        )

    def send28(k):
        def one(j, carry):
            @pl.when(j != dp)
            def _():
                rcopy(P28.at[k, j], R28.at[k, dp], cs.at[k, 0], cr.at[k, 0], (j, t)).start()

            return carry

        lax.fori_loop(0, 28, one, 0)

        @pl.when(dp < 28)
        def _():
            R28[k, dp] = P28[k, dp]

    def reduce28(k):
        @pl.when(dp < 28)
        def _():
            drain(R28.at[k, pl.ds(0, 31)], cr.at[k, 0])
            L28[k, dp] = jnp.sum(R28[k], axis=0)

            def one(j, carry):
                @pl.when(j != dp)
                def _():
                    rcopy(L28.at[k, dp], L28.at[k, dp], cs.at[k, 1], cr.at[k, 1], (j, t)).start()

                return carry

            lax.fori_loop(0, NDP, one, 0)

    def end28(k):
        @pl.when(dp < 28)
        def _():
            drain(L28.at[k, pl.ds(0, 27)], cr.at[k, 1])

        @pl.when(dp >= 28)
        def _():
            drain(L28.at[k, pl.ds(0, 28)], cr.at[k, 1])

    def send8(k):
        def one(j, carry):
            @pl.when(j != t)
            def _():
                rcopy(P8.at[k, j], R8T.at[k, t], cs.at[k, 2], cr.at[k, 2], (dp, j)).start()

            return carry

        lax.fori_loop(0, 8, one, 0)

        @pl.when(t < 8)
        def _():
            R8T[k, t] = P8[k, t]

    def middle8(k):
        @pl.when(t < 8)
        def _():
            drain(R8T.at[k, pl.ds(0, 15)], cr.at[k, 2])
            R8D[k, dp] = jnp.sum(R8T[k], axis=0)

            def one(j, carry):
                @pl.when(j != dp)
                def _():
                    rcopy(R8D.at[k, dp], R8D.at[k, dp], cs.at[k, 3], cr.at[k, 3], (j, t)).start()

                return carry

            lax.fori_loop(0, NDP, one, 0)

    def reduce8(k):
        @pl.when(t < 8)
        def _():
            drain(R8D.at[k, pl.ds(0, 31)], cr.at[k, 3])
            L8[k, t] = jnp.sum(R8D[k], axis=0)

            def one(j, carry):
                @pl.when(j != t)
                def _():
                    rcopy(L8.at[k, t], L8.at[k, t], cs.at[k, 4], cr.at[k, 4], (dp, j)).start()

                return carry

            lax.fori_loop(0, NT, one, 0)

    def end8(k):
        @pl.when(t < 8)
        def _():
            drain(L8.at[k, pl.ds(0, 7)], cr.at[k, 4])

        @pl.when(t >= 8)
        def _():
            drain(L8.at[k, pl.ds(0, 8)], cr.at[k, 4])

    put8(0, dot_nn(MU[...], uq[...], HI).T)
    send8(0)
    put28(0, dot_nn(MD[...], dq[...], HI).T)
    send28(0)

    def h_copy(i):
        own = HG.at[x]
        src = (own, own, HG.at[xl, top], HG.at[xrr, bot])[i]
        return rcopy(src, src, hs.at[i], hr.at[i], at_x(xrr if i % 2 == 0 else xl))

    def h_wait(i):
        x2 = wrap(x + 2, NX)
        ref = (HG.at[xl], HG.at[xrr], HG.at[x2, top], HG.at[x2, bot])[i]
        rcopy(ref, ref, hs.at[i], hr.at[i], (dp, t)).wait_recv()

    h_copy(0).start()
    h_copy(1).start()
    middle8(0)
    reduce28(0)
    h_wait(0)
    h_copy(2).start()
    h_wait(1)
    h_copy(3).start()
    reduce8(0)

    end28(0)
    down_sum = get(L28, 0, 7)
    put8(1, dot_nn(down_sum, MD[...], HI))
    send8(1)
    gram_part = dot_nt(down_sum, down_sum, HI)
    GR[t] = jnp.concatenate([gram_part[8 * g : 8 * g + 8] for g in range(4)], axis=1)

    def gram_send(j, carry):
        @pl.when(j != t)
        def _():
            rcopy(GR.at[t], GR.at[t], gs.at[0], gr.at[0], (dp, j)).start()

        return carry

    lax.fori_loop(0, NT, gram_send, 0)

    end8(0)
    up_sum = get(L8, 0, 2)
    put28(1, dot_nn(up_sum, MU[...], HI))
    send28(1)

    h_wait(2)
    h_wait(3)

    def ig_one(i, carry):
        IGP[i] = dot_nt(HG[i], WU[...].reshape(NZ * 128, WU.shape[2])).astype(BF16)
        return carry

    lax.fori_loop(0, NX, ig_one, 0)
    other = IGP.at[pl.ds(2 - 2 * c, 2)]
    pair_copy = rcopy(other, IGX, ps_s.at[0], ps_r.at[0], sib)
    pair_copy.start()

    middle8(1)
    up_inv = inverse_factor(dot_nt(up_sum, up_sum, HI))
    up_left_t = dot_nn(up_inv, up_sum, HI)
    up_left = up_left_t.T
    ul_out[...] = up_left
    reduce28(1)

    pair_copy.wait_recv()
    for i in range(2):
        both = (IGP[2 * c + i].astype(F32) + IGX[i].astype(F32)).astype(BF16)
        for k in range(NY):
            PS[k, i] = both[:, k * 128 : (k + 1) * 128]
    RY[y] = PS[y]

    def ry_send(j, carry):
        @pl.when(j != y)
        def _():
            rcopy(PS.at[j], RY.at[y], ry_s.at[0], ry_r.at[0], (dp, 2 * j + c)).start()

        return carry

    lax.fori_loop(0, NY, ry_send, 0)

    reduce8(1)
    drain(GR.at[pl.ds(0, NT - 1)], gr.at[0])
    packed = jnp.sum(GR[...], axis=0)
    gram = jnp.concatenate([packed[:, 32 * g : 32 * g + 32] for g in range(4)], axis=0)
    down_inv = inverse_factor(gram)
    down_left = dot_nn(down_inv, down_sum, HI).T
    dl_out[...] = down_left

    end28(1)
    up_right_t = dot_nn(up_inv, get(L28, 1, 7), HI) * (1.0 / NDP)
    ur_out[...] = up_right_t.T
    MU[...] -= dot_nn(up_left, up_right_t, HI)
    store_u = pltpu.make_async_copy(MU, uerr.at[0], err_sem.at[0])
    store_u.start()

    end8(1)
    down_right_t = dot_nn(down_inv, get(L8, 1, 2), HI) * (1.0 / NDP)
    dr_out[...] = down_right_t.T
    MD[...] -= dot_nn(down_left, down_right_t, HI)
    store_d = pltpu.make_async_copy(MD, derr.at[0], err_sem.at[1])
    store_d.start()

    drain(RY.at[pl.ds(0, NY - 1)], ry_r.at[0])
    for i in range(2):
        FY[i] = jnp.sum(RY[:, i].astype(F32), axis=0).astype(BF16)

    def last(i, h):
        return rcopy(
            FY.at[i],
            IGO.at[h],
            fs.at[i],
            fr.at[h],
            (z * NX + 2 * c + i, 2 * y + x // 2),
        )

    for h in range(2):
        for i in range(2):

            @pl.when(jnp.logical_and(lax.rem(x, 2) == h, foreign(i)))
            def _():
                last(i, h).start()

        @pl.when(jnp.logical_and(mine, lax.rem(x, 2) == h))
        def _():
            IGO[h] = FY[h]

    for h in range(2):

        @pl.when(foreign(h))
        def _():
            rcopy(IGO.at[h], IGO.at[h], fs.at[h], fr.at[h], (dp, t)).wait_recv()

        ig_out[:, h * 128 : (h + 1) * 128] = IGO[h]

    for mat in range(2):
        for step in range(1, 5):
            for way, half in ring_parts(step):
                ring(mat, way, step, half).wait_send()
        for i in range(6):
            rs_copy(mat, i).wait_send()
    for arr in range(2):
        for h in range(2):

            @pl.when(foreign(h))
            def _():
                piece(arr, h).wait_send()

        for off in range(1, NY):
            spread(arr, off).wait_send()
        for off in range(NY):
            to_sibling(arr, wrap(y - off, NY), off).wait_send()

    @pl.when(t == 0)
    def _():
        for arr in range(2):

            def one(j, carry):
                rcopy(WIN.at[arr], WIN.at[arr], ws.at[arr], wr.at[arr], (dp, j)).wait_send()
                return carry

            lax.fori_loop(1, NT, one, 0)

    for i in range(4):
        h_copy(i).wait_send()
    pair_copy.wait_send()
    drain(PS.at[pl.ds(0, NY - 1)], ry_s.at[0])
    for i in range(2):

        @pl.when(foreign(i))
        def _():
            rcopy(FY.at[i], FY.at[i], fs.at[i], fr.at[i], (dp, t)).wait_send()

    for k in range(2):

        @pl.when(dp < 28)
        def _():
            drain(P28.at[k, pl.ds(0, 27)], cs.at[k, 0])
            drain(R28.at[k, pl.ds(0, 31)], cs.at[k, 1])

        @pl.when(dp >= 28)
        def _():
            drain(P28.at[k, pl.ds(0, 28)], cs.at[k, 0])

        @pl.when(t < 8)
        def _():
            drain(P8.at[k, pl.ds(0, 7)], cs.at[k, 2])
            drain(R8D.at[k, pl.ds(0, 31)], cs.at[k, 3])
            drain(R8T.at[k, pl.ds(0, 15)], cs.at[k, 4])

        @pl.when(t >= 8)
        def _():
            drain(P8.at[k, pl.ds(0, 8)], cs.at[k, 2])

    drain(GR.at[pl.ds(0, NT - 1)], gs.at[0])
    store_u.wait()
    store_d.wait()


def shards(tokens, out_grad, up_weight, down_weight, up_accum, down_accum, up_q, down_q):
    rows, feats = tokens.shape
    hid = up_weight.shape[1]
    win = up_accum.shape[1]
    rank = up_q.shape[1]
    quarter = NZ * 128
    vmem = pl.BlockSpec(memory_space=pltpu.VMEM)
    hbm = pl.BlockSpec(memory_space=pl.ANY)
    sem = pltpu.SemaphoreType.DMA
    V = pltpu.VMEM
    shape = jax.ShapeDtypeStruct
    outs = pl.pallas_call(
        kernel,
        out_shape=[
            shape((rows, feats), BF16),
            shape((win, rank), F32),
            shape((hid, rank), F32),
            shape((hid, rank), F32),
            shape((win, rank), F32),
            shape(up_accum.shape, F32),
            shape(down_accum.shape, F32),
        ],
        in_specs=[vmem] * 6 + [hbm] * 2,
        out_specs=[vmem] * 5 + [hbm] * 2,
        scratch_shapes=[
            V((2, NX, rows, quarter), BF16),
            V((NZ, 128, hid), BF16),
            V((hid, quarter), BF16),
            V((2, rows, win), BF16),
            V((2, NX, rows, hid), F32),
            V((2, 3, rows, hid), BF16),
            V((2, 2, rows // 2, hid), BF16),
            V((2, 2, rows, hid), BF16),
            V((NX, rows, hid), BF16),
            V((NX, rows, quarter), BF16),
            V((2, rows, quarter), BF16),
            V((NY, 2, rows, 128), BF16),
            V((NY, 2, rows, 128), BF16),
            V((2, rows, 128), BF16),
            V((2, rows, 128), BF16),
            V((win, hid), F32),
            V((hid, win), F32),
            V((2, 28, 8, 128), F32),
            V((2, NDP, 8, 128), F32),
            V((2, 28, 8, 128), F32),
            V((2, 8, 8, 128), F32),
            V((2, NT, 8, 128), F32),
            V((2, NDP, 8, 128), F32),
            V((2, 8, 8, 128), F32),
            V((NT, 8, 128), F32),
            sem((2,)),
            sem((2,)),
            sem((2, 2, 2, 4)),
            sem((2, 2, 2, 4)),
            sem((2, 2)),
            sem((2, 2)),
            sem((2, NY)),
            sem((2, NY)),
            sem((2, NY)),
            sem((2, NY)),
            sem((2,)),
            sem((2,)),
            sem((2, 6)),
            sem((2, 6)),
            sem((4,)),
            sem((4,)),
            sem((1,)),
            sem((1,)),
            sem((1,)),
            sem((1,)),
            sem((2,)),
            sem((2,)),
            sem((2, 5)),
            sem((2, 5)),
            sem((1,)),
            sem((1,)),
        ],
        compiler_params=pltpu.CompilerParams(
            collective_id=0, has_side_effects=True, vmem_limit_bytes=56 * 1024 * 1024
        ),
    )(tokens, out_grad, up_weight, down_weight, up_q, down_q, up_accum, down_accum)
    input_grad, up_left, up_right, down_left, down_right, up_error, down_error = outs
    return input_grad, up_error, up_left, up_right, down_error, down_left, down_right


def solution(mesh):
    return jax.shard_map(
        shards,
        mesh=mesh,
        in_specs=(
            P("dp", "tensor"),
            P("dp", "tensor"),
            P("dp", "tensor"),
            P("tensor", "dp"),
            P("dp", None, "tensor"),
            P("dp", "tensor", None),
            P("tensor", None),
            P(),
        ),
        out_specs=(
            P("dp", "tensor"),
            P("dp", None, "tensor"),
            P(),
            P("tensor", None),
            P("dp", "tensor", None),
            P("tensor", None),
            P(),
        ),
        check_vma=False,
    )
```

```python
import functools
import math

import jax
import jax.numpy as jnp
from jax import lax
from jax.experimental import pallas as pl
from jax.experimental.pallas import tpu as pltpu
from jax.sharding import PartitionSpec as P

MESH = pl.DeviceIdType.MESH
HI = lax.Precision.HIGHEST
NZ, NX, NY = 8, 4, 8
NDP, NT = 32, 16
F32, BF16 = jnp.float32, jnp.bfloat16


def wrap(a, n):
    return lax.rem(a + 4 * n, n)


def dot_nt(a, b, precision=None):
    return lax.dot_general(
        a, b, (((1,), (1,)), ((), ())), preferred_element_type=F32, precision=precision
    )


def dot_nn(a, b, precision=None):
    return jnp.dot(a, b, preferred_element_type=F32, precision=precision)


def inverse_factor(gram):
    n = gram.shape[0]
    rows = lax.broadcasted_iota(jnp.int32, (n, 128), 0)
    lanes = lax.broadcasted_iota(jnp.int32, (n, 128), 1)
    unit = jnp.where(lanes == rows + n, 1.0, 0.0).astype(F32)
    work = jnp.concatenate([gram, jnp.zeros((n, 128 - n), F32)], axis=1) + unit
    for k in range(n):
        scale = lax.rsqrt(work[k : k + 1, k : k + 1])
        line = work[k : k + 1, :] * scale
        col = work[:, k : k + 1] * scale
        work = jnp.where(rows > k, work - col * line, jnp.where(rows == k, line, work))
    return work[:, n : 2 * n]


GROUPS = ((0, 512), (512, 384))


def kernel(
    tok_in, og_in, wu_in, wd_in, uq_in, dq_in, uacc, dacc,
    ig_out, ul_out, ur_out, dl_out, dr_out, mu_out, md_out,
    TO, UQ, DQ, AU, AD, GQ, UL, UR, DL, DR,
    A, WU, WD, WIN, PF, SB, FB, RB, HG, IGP, IGX, PS, RY, FY, IGO, MU, MD,
    P28, R28, L28, P8, R8T, R8D, L8, GR,
    in_sem, acc_sem, out_sem, ring_s, ring_r, xs, xr, ys, yr, ds, dr, ws, wr,
    rs_s, rs_r, hs, hr, ps_s, ps_r, ry_s, ry_r, fs, fr, cs, cr, gs, gr,
):
    dp, t = lax.axis_index("dp"), lax.axis_index("tensor")
    z, x = dp // NX, lax.rem(dp, NX)
    y, c = t // 2, lax.rem(t, 2)
    mine = x // 2 == c
    xl, xrr = wrap(x - 1, NX), wrap(x + 1, NX)
    sib = (dp, t + 1 - 2 * c)
    tok, og = TO.at[0], TO.at[1]
    tokens = TO.shape[1]
    grad_scale = 1.0 / math.sqrt(tokens)

    def lanes_of(i):
        return pl.ds(pl.multiple_of(i * 128, 128), 128)

    def rcopy(src, dst, s, r, dev):
        return pltpu.make_async_remote_copy(
            src_ref=src, dst_ref=dst, send_sem=s, recv_sem=r, device_id=dev, device_id_type=MESH
        )

    def drain(ref, sem):
        pltpu.make_async_copy(ref, ref, sem).wait()

    def at_x(xi):
        return (z * NX + xi, t)

    loads = [
        pltpu.make_async_copy(src, dst, in_sem.at[i])
        for i, (src, dst) in enumerate(
            (
                (wu_in, WU.at[z]),
                (wd_in, WD.at[:, lanes_of(z)]),
                (tok_in, tok),
                (og_in, og),
                (uq_in, UQ),
                (dq_in, DQ),
            )
        )
    ]
    load_u = pltpu.make_async_copy(uacc.at[0], MU, acc_sem.at[0])
    load_d = pltpu.make_async_copy(dacc.at[0], MD, acc_sem.at[1])
    for load in loads:
        load.start()
    load_u.start()
    load_d.start()

    barrier = pltpu.get_barrier_semaphore()

    def greet_dp(j, carry):
        @pl.when(j != dp)
        def _():
            pl.semaphore_signal(barrier, inc=1, device_id=(j, t), device_id_type=MESH)

        return carry

    def greet_t(j, carry):
        @pl.when(j != t)
        def _():
            pl.semaphore_signal(barrier, inc=1, device_id=(dp, j), device_id_type=MESH)

        return carry

    lax.fori_loop(0, NDP, greet_dp, 0)
    lax.fori_loop(0, NT, greet_t, 0)

    @pl.when(jnp.logical_not(mine))
    def _():
        for h in range(2):
            pl.semaphore_signal(
                barrier,
                inc=1,
                device_id=(z * NX + 2 * c + h, 2 * y + x // 2),
                device_id_type=MESH,
            )

    pl.semaphore_wait(barrier, NDP + NT - 2 + 2 * jnp.where(mine, 0, 1).astype(jnp.int32))

    for load in loads[:4]:
        load.wait()
    for h in range(2):

        @pl.when(jnp.logical_and(mine, lax.rem(x, 2) == h))
        def _():
            for arr in range(2):
                A[arr, x, :, lanes_of(y)] = TO[arr, :, h * 128 : (h + 1) * 128]

    @pl.when(t == 0)
    def _():
        WIN[...] = TO[...]

    def slot(mat, zi, g):
        hidden_range = pl.ds(*GROUPS[g])
        if mat == 0:
            return WU.at[zi, :, hidden_range]
        return WD.at[hidden_range, lanes_of(zi)]

    def ring(mat, way, step, g):
        if way == 0:
            zi, to = wrap(z - step + 1, NZ), wrap(z + 1, NZ)
        else:
            zi, to = wrap(z + step - 1, NZ), wrap(z - 1, NZ)
        i = (mat, way, g, step - 1)
        ref = slot(mat, zi, g)
        return rcopy(ref, ref, ring_s.at[i], ring_r.at[i], (to * NX + x, t))

    def ring_ways(step, g):
        return (0, 1) if step < 4 else (g,)

    def ring_send(mat, step, g):
        for way in ring_ways(step, g):
            ring(mat, way, step, g).start()

    def ring_arrived(mat, way, step, g):
        zi = wrap(z - step, NZ) if way == 0 else wrap(z + step, NZ)
        ref = slot(mat, zi, g)
        i = (mat, way, g, step - 1)
        rcopy(ref, ref, ring_s.at[i], ring_r.at[i], (dp, t)).wait_recv()

    def ring_pass(mat, step, g):
        for way in ring_ways(step - 1, g):
            ring_arrived(mat, way, step - 1, g)
            if way in ring_ways(step, g):
                ring(mat, way, step, g).start()

    def ring_end(mat, g):
        for way in ring_ways(4, g):
            ring_arrived(mat, way, 4, g)

    ring_send(0, 1, 0)
    ring_send(1, 1, 0)

    def piece(arr, h):
        xd = 2 * c + h
        src = TO.at[arr, :, pl.ds(h * 128, 128)]
        return rcopy(
            src,
            A.at[arr, x, :, lanes_of(y)],
            xs.at[arr, h],
            xr.at[arr, lax.rem(x, 2)],
            (z * NX + xd, 2 * y + x // 2),
        )

    def foreign(h):
        return jnp.logical_not(jnp.logical_and(mine, lax.rem(x, 2) == h))

    for arr in range(2):
        for h in range(2):

            @pl.when(foreign(h))
            def _():
                piece(arr, h).start()

    def pair(arr, yi):
        return A.at[arr, pl.ds(2 * c, 2), :, lanes_of(yi)]

    def spread(arr, off):
        yd = wrap(y + off, NY)
        return rcopy(pair(arr, y), pair(arr, y), ys.at[arr, off], yr.at[arr, off], (dp, 2 * yd + c))

    def to_sibling(arr, yi, off):
        return rcopy(pair(arr, yi), pair(arr, yi), ds.at[arr, off], dr.at[arr, off], sib)

    for arr in range(2):
        for h in range(2):

            @pl.when(foreign(h))
            def _():
                ref = A.at[arr, 2 * c + h, :, lanes_of(y)]
                rcopy(ref, ref, xs.at[arr, h], xr.at[arr, h], (dp, t)).wait_recv()

        for off in (4, 3, 5, 2, 6, 1, 7):
            spread(arr, off).start()
        to_sibling(arr, y, 0).start()

    @pl.when(t == 0)
    def _():
        def one(j, carry):
            rcopy(tok, WIN.at[0], ws.at[0], wr.at[0], (dp, j)).start()
            rcopy(og, WIN.at[1], ws.at[1], wr.at[1], (dp, j)).start()
            return carry

        lax.fori_loop(1, NT, one, 0)

    def y_arrivals(arr):
        for off in (1, 7, 2, 6, 3, 5, 4):
            yi = wrap(y - off, NY)
            ref = pair(arr, yi)
            rcopy(ref, ref, ys.at[arr, off], yr.at[arr, off], (dp, t)).wait_recv()
            to_sibling(arr, yi, off).start()

    def sibling_arrivals(arr):
        for off in range(NY):
            yi = wrap(y - off, NY)
            ref = A.at[arr, pl.ds(2 - 2 * c, 2), :, lanes_of(yi)]
            rcopy(ref, ref, ds.at[arr, off], dr.at[arr, off], (dp, t)).wait_recv()

    def products(mat, g):
        lo, size = GROUPS[g]
        cols = slice(lo, lo + size)

        def one(d, carry):
            xi = wrap(x + d, NX)
            if mat == 0:
                PF[0, d, :, cols] = dot_nn(A[0, xi], WU[:, :, cols].reshape(NZ * 128, size))
            else:
                PF[1, d, :, cols] = dot_nt(A[1, xi], WD[cols, :])
            return carry

        lax.fori_loop(0, NX, one, 0)

    half_rows = tokens // 2
    top, bot = pl.ds(0, half_rows), pl.ds(half_rows, half_rows)

    def rs_copy(mat, g, i):
        cols = pl.ds(*GROUPS[g])
        src = (SB.at[mat, 1, top, cols], SB.at[mat, 1, bot, cols], SB.at[mat, 0, bot, cols],
               SB.at[mat, 2, top, cols], SB.at[mat, 0, top, cols], SB.at[mat, 2, bot, cols])[i]
        dst = (FB.at[mat, 0, :, cols], FB.at[mat, 1, :, cols], RB.at[mat, 0, bot, cols],
               RB.at[mat, 1, top, cols], RB.at[mat, 0, top, cols], RB.at[mat, 1, bot, cols])[i]
        to = at_x(xrr if i % 2 == 0 else xl)
        return rcopy(src, dst, rs_s.at[mat, g, i], rs_r.at[mat, g, i], to)

    def rs_first(mat, g):
        cols = slice(GROUPS[g][0], sum(GROUPS[g]))
        SB[mat, 1, :, cols] = PF[mat, 2, :, cols].astype(BF16)
        rs_copy(mat, g, 0).start()
        rs_copy(mat, g, 1).start()
        SB[mat, 0, half_rows:, cols] = PF[mat, 1, half_rows:, cols].astype(BF16)
        rs_copy(mat, g, 2).start()
        SB[mat, 2, :half_rows, cols] = PF[mat, 3, :half_rows, cols].astype(BF16)
        rs_copy(mat, g, 3).start()

    def rs_second(mat, g):
        cols = slice(GROUPS[g][0], sum(GROUPS[g]))
        rs_copy(mat, g, 0).wait_recv()
        SB[mat, 0, :half_rows, cols] = (
            PF[mat, 1, :half_rows, cols] + FB[mat, 0, :, cols].astype(F32)
        ).astype(BF16)
        rs_copy(mat, g, 4).start()
        rs_copy(mat, g, 1).wait_recv()
        SB[mat, 2, half_rows:, cols] = (
            PF[mat, 3, half_rows:, cols] + FB[mat, 1, :, cols].astype(F32)
        ).astype(BF16)
        rs_copy(mat, g, 5).start()

    def rs_end(mat, g):
        for i in range(2, 6):
            rs_copy(mat, g, i).wait_recv()

    ring_pass(0, 2, 0)
    ring_pass(1, 2, 0)
    loads[4].wait()
    load_u.wait()
    AU[...] = dot_nt(UQ[...], MU[...], HI)
    ring_pass(0, 3, 0)
    ring_pass(1, 3, 0)
    ring_send(0, 1, 1)
    loads[5].wait()
    load_d.wait()
    AD[...] = dot_nt(DQ[...], MD[...], HI)
    ring_pass(0, 4, 0)
    ring_pass(1, 4, 0)
    ring_send(1, 1, 1)
    y_arrivals(0)
    ring_pass(0, 2, 1)
    ring_end(0, 0)
    sibling_arrivals(0)
    products(0, 0)
    rs_first(0, 0)
    ring_pass(1, 2, 1)
    y_arrivals(1)
    ring_pass(0, 3, 1)
    ring_end(1, 0)
    sibling_arrivals(1)
    products(1, 0)
    rs_first(1, 0)
    rs_second(0, 0)
    ring_pass(1, 3, 1)
    rs_second(1, 0)

    @pl.when(t != 0)
    def _():
        for arr in range(2):
            rcopy(WIN.at[arr], WIN.at[arr], ws.at[arr], wr.at[arr], (dp, t)).wait_recv()

    ring_pass(0, 4, 1)
    ring_pass(1, 4, 1)
    GQ[...] = dot_nt(DQ[...], WIN[1].astype(F32), HI)
    rs_end(0, 0)
    ring_end(0, 1)
    products(0, 1)
    rs_first(0, 1)
    ring_end(1, 1)
    products(1, 1)
    rs_first(1, 1)
    rs_second(0, 1)
    rs_end(1, 0)
    rs_end(0, 1)
    rs_second(1, 1)
    rs_end(1, 1)
    preact = PF[0, 0] + RB[0, 0].astype(F32) + RB[0, 1].astype(F32)
    back = PF[1, 0] + RB[1, 0].astype(F32) + RB[1, 1].astype(F32)
    squash = jax.nn.sigmoid(preact)
    act = (preact * squash).astype(BF16)
    hidden = (back * squash * (1.0 + preact * (1.0 - squash))).astype(BF16)
    HG[x] = hidden

    def put28(k, arr):
        for g in range(4):
            for l in range(7):
                P28[k, g * 7 + l] = arr[8 * g : 8 * g + 8, 128 * l : 128 * l + 128]

    def put8(k, arr):
        for g in range(4):
            for l in range(2):
                P8[k, g * 2 + l] = arr[8 * g : 8 * g + 8, 128 * l : 128 * l + 128]

    def get(buf, k, n):
        return jnp.concatenate(
            [jnp.concatenate([buf[k, g * n + l] for l in range(n)], axis=1) for g in range(4)],
            axis=0,
        )

    def send28(k):
        def one(j, carry):
            @pl.when(j != dp)
            def _():
                rcopy(P28.at[k, j], R28.at[k, dp], cs.at[k, 0], cr.at[k, 0], (j, t)).start()

            return carry

        lax.fori_loop(0, 28, one, 0)

        @pl.when(dp < 28)
        def _():
            R28[k, dp] = P28[k, dp]

    def reduce28(k):
        @pl.when(dp < 28)
        def _():
            drain(R28.at[k, pl.ds(0, 31)], cr.at[k, 0])
            L28[k, dp] = jnp.sum(R28[k], axis=0)

            def one(j, carry):
                @pl.when(j != dp)
                def _():
                    rcopy(L28.at[k, dp], L28.at[k, dp], cs.at[k, 1], cr.at[k, 1], (j, t)).start()

                return carry

            lax.fori_loop(0, NDP, one, 0)

    def end28(k):
        @pl.when(dp < 28)
        def _():
            drain(L28.at[k, pl.ds(0, 27)], cr.at[k, 1])

        @pl.when(dp >= 28)
        def _():
            drain(L28.at[k, pl.ds(0, 28)], cr.at[k, 1])

    def send8(k):
        def one(j, carry):
            @pl.when(j != t)
            def _():
                rcopy(P8.at[k, j], R8T.at[k, t], cs.at[k, 2], cr.at[k, 2], (dp, j)).start()

            return carry

        lax.fori_loop(0, 8, one, 0)

        @pl.when(t < 8)
        def _():
            R8T[k, t] = P8[k, t]

    def middle8(k):
        @pl.when(t < 8)
        def _():
            drain(R8T.at[k, pl.ds(0, 15)], cr.at[k, 2])
            R8D[k, dp] = jnp.sum(R8T[k], axis=0)

            def one(j, carry):
                @pl.when(j != dp)
                def _():
                    rcopy(R8D.at[k, dp], R8D.at[k, dp], cs.at[k, 3], cr.at[k, 3], (j, t)).start()

                return carry

            lax.fori_loop(0, NDP, one, 0)

    def reduce8(k):
        @pl.when(t < 8)
        def _():
            drain(R8D.at[k, pl.ds(0, 31)], cr.at[k, 3])
            L8[k, t] = jnp.sum(R8D[k], axis=0)

            def one(j, carry):
                @pl.when(j != t)
                def _():
                    rcopy(L8.at[k, t], L8.at[k, t], cs.at[k, 4], cr.at[k, 4], (dp, j)).start()

                return carry

            lax.fori_loop(0, NT, one, 0)

    def end8(k):
        @pl.when(t < 8)
        def _():
            drain(L8.at[k, pl.ds(0, 7)], cr.at[k, 4])

        @pl.when(t >= 8)
        def _():
            drain(L8.at[k, pl.ds(0, 8)], cr.at[k, 4])

    hq = dot_nt(UQ[...], hidden.astype(F32), HI)
    put8(0, AU[...] + dot_nn(hq, WIN[0].astype(F32), HI) * grad_scale)
    send8(0)
    put28(0, AD[...] + dot_nn(GQ[...], act.astype(F32), HI) * grad_scale)
    send28(0)

    def h_copy(i):
        own = HG.at[x]
        src = (own, own, HG.at[xl, top], HG.at[xrr, bot])[i]
        return rcopy(src, src, hs.at[i], hr.at[i], at_x(xrr if i % 2 == 0 else xl))

    def h_wait(i):
        x2 = wrap(x + 2, NX)
        ref = (HG.at[xl], HG.at[xrr], HG.at[x2, top], HG.at[x2, bot])[i]
        rcopy(ref, ref, hs.at[i], hr.at[i], (dp, t)).wait_recv()

    def ig_product(i):
        IGP[i] = dot_nt(HG[i], WU[...].reshape(NZ * 128, WU.shape[2])).astype(BF16)

    h_copy(0).start()
    h_copy(1).start()
    MU[...] += dot_nn(WIN[0].T, hidden) * grad_scale
    MD[...] += dot_nn(act.T, WIN[1]) * grad_scale
    store_u = pltpu.make_async_copy(MU, mu_out, acc_sem.at[0])
    store_d = pltpu.make_async_copy(MD, md_out, acc_sem.at[1])
    store_u.start()
    store_d.start()
    middle8(0)
    reduce28(0)
    h_wait(0)
    h_copy(2).start()
    h_wait(1)
    h_copy(3).start()

    def ig_near(d, carry):
        ig_product(wrap(x + d - 1, NX))
        return carry

    lax.fori_loop(0, 3, ig_near, 0)
    reduce8(0)
    h_wait(2)
    h_wait(3)
    lax.fori_loop(3, 4, ig_near, 0)
    other = IGP.at[pl.ds(2 - 2 * c, 2)]
    pair_copy = rcopy(other, IGX, ps_s.at[0], ps_r.at[0], sib)
    pair_copy.start()

    end28(0)
    down_sum = get(L28, 0, 7)
    put8(1, dot_nn(down_sum, MD[...], HI))
    send8(1)
    gram_part = dot_nt(down_sum, down_sum, HI)
    GR[t] = jnp.concatenate([gram_part[8 * g : 8 * g + 8] for g in range(4)], axis=1)

    def gram_send(j, carry):
        @pl.when(j != t)
        def _():
            rcopy(GR.at[t], GR.at[t], gs.at[0], gr.at[0], (dp, j)).start()

        return carry

    lax.fori_loop(0, NT, gram_send, 0)

    pair_copy.wait_recv()
    for i in range(2):
        both = (IGP[2 * c + i].astype(F32) + IGX[i].astype(F32)).astype(BF16)
        for k in range(NY):
            PS[k, i] = both[:, k * 128 : (k + 1) * 128]
    RY[y] = PS[y]

    def ry_send(off, carry):
        j = wrap(y + off, NY)
        rcopy(PS.at[j], RY.at[y], ry_s.at[0], ry_r.at[0], (dp, 2 * j + c)).start()
        return carry

    lax.fori_loop(1, NY, ry_send, 0)

    end8(0)
    up_sum = get(L8, 0, 2)
    put28(1, dot_nn(up_sum, MU[...], HI))
    send28(1)
    middle8(1)

    def put_out(ref, value, dst, i):
        ref[...] = value
        copy = pltpu.make_async_copy(ref, dst, out_sem.at[i])
        copy.start()
        return copy

    results = []
    up_inv = inverse_factor(dot_nt(up_sum, up_sum, HI))
    results.append(put_out(UL, dot_nn(up_inv, up_sum, HI), ul_out, 0))
    reduce28(1)
    drain(GR.at[pl.ds(0, NT - 1)], gr.at[0])
    packed = jnp.sum(GR[...], axis=0)
    gram = jnp.concatenate([packed[:, 32 * g : 32 * g + 32] for g in range(4)], axis=0)
    reduce8(1)
    down_inv = inverse_factor(gram)
    results.append(put_out(DL, dot_nn(down_inv, down_sum, HI), dl_out, 1))

    drain(RY.at[pl.ds(0, NY - 1)], ry_r.at[0])
    for i in range(2):
        FY[i] = jnp.sum(RY[:, i].astype(F32), axis=0).astype(BF16)

    def last(i, h):
        return rcopy(
            FY.at[i],
            IGO.at[h],
            fs.at[i],
            fr.at[h],
            (z * NX + 2 * c + i, 2 * y + x // 2),
        )

    for h in range(2):
        for i in range(2):

            @pl.when(jnp.logical_and(lax.rem(x, 2) == h, foreign(i)))
            def _():
                last(i, h).start()

        @pl.when(jnp.logical_and(mine, lax.rem(x, 2) == h))
        def _():
            IGO[h] = FY[h]

    end28(1)
    results.append(
        put_out(UR, dot_nn(up_inv, get(L28, 1, 7), HI) * (1.0 / NDP), ur_out, 2)
    )
    for h in range(2):

        @pl.when(foreign(h))
        def _():
            rcopy(IGO.at[h], IGO.at[h], fs.at[h], fr.at[h], (dp, t)).wait_recv()

        copy = pltpu.make_async_copy(
            IGO.at[h], ig_out.at[:, pl.ds(h * 128, 128)], out_sem.at[4 + h]
        )
        copy.start()
        results.append(copy)
    end8(1)
    results.append(
        put_out(DR, dot_nn(down_inv, get(L8, 1, 2), HI) * (1.0 / NDP), dr_out, 3)
    )

    for mat in range(2):
        for g in range(2):
            for step in range(1, 5):
                for way in ring_ways(step, g):
                    ring(mat, way, step, g).wait_send()
            for i in range(6):
                rs_copy(mat, g, i).wait_send()
    for arr in range(2):
        for h in range(2):

            @pl.when(foreign(h))
            def _():
                piece(arr, h).wait_send()

        for off in range(1, NY):
            spread(arr, off).wait_send()
        for off in range(NY):
            to_sibling(arr, wrap(y - off, NY), off).wait_send()

    @pl.when(t == 0)
    def _():
        for arr in range(2):

            def one(j, carry):
                rcopy(WIN.at[arr], WIN.at[arr], ws.at[arr], wr.at[arr], (dp, j)).wait_send()
                return carry

            lax.fori_loop(1, NT, one, 0)

    for i in range(4):
        h_copy(i).wait_send()
    pair_copy.wait_send()
    drain(PS.at[pl.ds(0, NY - 1)], ry_s.at[0])
    for i in range(2):

        @pl.when(foreign(i))
        def _():
            rcopy(FY.at[i], FY.at[i], fs.at[i], fr.at[i], (dp, t)).wait_send()

    for k in range(2):

        @pl.when(dp < 28)
        def _():
            drain(P28.at[k, pl.ds(0, 27)], cs.at[k, 0])
            drain(R28.at[k, pl.ds(0, 31)], cs.at[k, 1])

        @pl.when(dp >= 28)
        def _():
            drain(P28.at[k, pl.ds(0, 28)], cs.at[k, 0])

        @pl.when(t < 8)
        def _():
            drain(P8.at[k, pl.ds(0, 7)], cs.at[k, 2])
            drain(R8D.at[k, pl.ds(0, 31)], cs.at[k, 3])
            drain(R8T.at[k, pl.ds(0, 15)], cs.at[k, 4])

        @pl.when(t >= 8)
        def _():
            drain(P8.at[k, pl.ds(0, 8)], cs.at[k, 2])

    drain(GR.at[pl.ds(0, NT - 1)], gs.at[0])
    store_u.wait()
    store_d.wait()
    for copy in results:
        copy.wait()


def finish(*refs):
    ins, outs, held = refs[:7], refs[7:14], refs[14:21]
    came, left = refs[21], refs[22]
    loads = [pltpu.make_async_copy(ins[i], held[i], came.at[i]) for i in range(7)]
    ends = [outs[i] if i < 5 else outs[i].at[0] for i in range(7)]
    stores = [pltpu.make_async_copy(held[i], ends[i], left.at[i]) for i in range(7)]
    for i in (1, 2, 5, 3, 4, 6, 0):
        loads[i].start()
    for i, low, high in ((5, 1, 2), (6, 3, 4)):
        for k in (low, high, i):
            loads[k].wait()
        held[i][...] -= dot_nn(held[low][...].T, held[high][...], HI)
        for k in (i, low, high):
            stores[k].start()
    loads[0].wait()
    stores[0].start()
    for store in stores:
        store.wait()


def shards(tokens, out_grad, up_weight, down_weight, up_accum, down_accum, up_q, down_q):
    rows, feats = tokens.shape
    hid = up_weight.shape[1]
    win = up_accum.shape[1]
    rank = up_q.shape[1]
    quarter = NZ * 128
    hbm = pl.BlockSpec(memory_space=pl.ANY)
    sem = pltpu.SemaphoreType.DMA
    V = pltpu.VMEM
    shape = jax.ShapeDtypeStruct
    outs = pl.pallas_call(
        kernel,
        out_shape=[
            shape((rows, feats), BF16),
            shape((rank, win), F32),
            shape((rank, hid), F32),
            shape((rank, hid), F32),
            shape((rank, win), F32),
            shape((win, hid), F32),
            shape((hid, win), F32),
        ],
        in_specs=[hbm] * 8,
        out_specs=[hbm] * 7,
        scratch_shapes=[
            V((2, rows, feats), BF16),
            V((rank, hid), F32),
            V((rank, win), F32),
            V((rank, win), F32),
            V((rank, hid), F32),
            V((rank, rows), F32),
            V((rank, win), F32),
            V((rank, hid), F32),
            V((rank, hid), F32),
            V((rank, win), F32),
            V((2, NX, rows, quarter), BF16),
            V((NZ, 128, hid), BF16),
            V((hid, quarter), BF16),
            V((2, rows, win), BF16),
            V((2, NX, rows, hid), F32),
            V((2, 3, rows, hid), BF16),
            V((2, 2, rows // 2, hid), BF16),
            V((2, 2, rows, hid), BF16),
            V((NX, rows, hid), BF16),
            V((NX, rows, quarter), BF16),
            V((2, rows, quarter), BF16),
            V((NY, 2, rows, 128), BF16),
            V((NY, 2, rows, 128), BF16),
            V((2, rows, 128), BF16),
            V((2, rows, 128), BF16),
            V((win, hid), F32),
            V((hid, win), F32),
            V((2, 28, 8, 128), F32),
            V((2, NDP, 8, 128), F32),
            V((2, 28, 8, 128), F32),
            V((2, 8, 8, 128), F32),
            V((2, NT, 8, 128), F32),
            V((2, NDP, 8, 128), F32),
            V((2, 8, 8, 128), F32),
            V((NT, 8, 128), F32),
            sem((6,)),
            sem((2,)),
            sem((6,)),
            sem((2, 2, 2, 4)),
            sem((2, 2, 2, 4)),
            sem((2, 2)),
            sem((2, 2)),
            sem((2, NY)),
            sem((2, NY)),
            sem((2, NY)),
            sem((2, NY)),
            sem((2,)),
            sem((2,)),
            sem((2, 2, 6)),
            sem((2, 2, 6)),
            sem((4,)),
            sem((4,)),
            sem((1,)),
            sem((1,)),
            sem((1,)),
            sem((1,)),
            sem((2,)),
            sem((2,)),
            sem((2, 5)),
            sem((2, 5)),
            sem((1,)),
            sem((1,)),
        ],
        compiler_params=pltpu.CompilerParams(
            collective_id=0, has_side_effects=True, vmem_limit_bytes=63 * 1024 * 1024
        ),
    )(tokens, out_grad, up_weight, down_weight, up_q.T, down_q.T, up_accum, down_accum)
    input_grad, ul, ur, dl, dr, mu, md = outs
    results = pl.pallas_call(
        finish,
        out_shape=[
            shape((rows, feats), BF16),
            shape((rank, win), F32),
            shape((rank, hid), F32),
            shape((rank, hid), F32),
            shape((rank, win), F32),
            shape(up_accum.shape, F32),
            shape(down_accum.shape, F32),
        ],
        in_specs=[hbm] * 7,
        out_specs=[hbm] * 7,
        scratch_shapes=[
            V((rows, feats), BF16),
            V((rank, win), F32),
            V((rank, hid), F32),
            V((rank, hid), F32),
            V((rank, win), F32),
            V((win, hid), F32),
            V((hid, win), F32),
            sem((7,)),
            sem((7,)),
        ],
        compiler_params=pltpu.CompilerParams(vmem_limit_bytes=63 * 1024 * 1024),
    )(input_grad, ul, ur, dl, dr, mu, md)
    input_grad, ul, ur, dl, dr, up_error, down_error = results
    return input_grad, up_error, ul.T, ur.T, down_error, dl.T, dr.T


def solution(mesh):
    return jax.shard_map(
        shards,
        mesh=mesh,
        in_specs=(
            P("dp", "tensor"),
            P("dp", "tensor"),
            P("dp", "tensor"),
            P("tensor", "dp"),
            P("dp", None, "tensor"),
            P("dp", "tensor", None),
            P("tensor", None),
            P(),
        ),
        out_specs=(
            P("dp", "tensor"),
            P("dp", None, "tensor"),
            P(),
            P("tensor", None),
            P("dp", "tensor", None),
            P("tensor", None),
            P(),
        ),
        check_vma=False,
    )
```

```python
import functools
import math

import jax
import jax.numpy as jnp
from jax import lax
from jax.experimental import pallas as pl
from jax.experimental.pallas import tpu as pltpu
from jax.sharding import PartitionSpec as P

MESH = pl.DeviceIdType.MESH
HI = lax.Precision.HIGHEST
NZ, NX, NY = 8, 4, 8
NDP, NT = 32, 16
F32, BF16 = jnp.float32, jnp.bfloat16


def wrap(a, n):
    return lax.rem(a + 4 * n, n)


def thirds(a):
    high = a.astype(BF16)
    rest = a - high.astype(F32)
    middle = rest.astype(BF16)
    return high, middle, (rest - middle.astype(F32)).astype(BF16)


def dot_thirds(left_t, right_t):
    lh, lm, ll = thirds(left_t)
    rh, rm, rl = thirds(right_t)
    left = jnp.concatenate([ll, lm, lh, lm, lh, lh], axis=0)
    right = jnp.concatenate([rh, rm, rl, rh, rm, rh], axis=0)
    return dot_nn(left.astype(F32).T.astype(BF16), right)


def dot_nt(a, b, precision=None):
    return lax.dot_general(
        a, b, (((1,), (1,)), ((), ())), preferred_element_type=F32, precision=precision
    )


def dot_nn(a, b, precision=None):
    return jnp.dot(a, b, preferred_element_type=F32, precision=precision)


def inverse_factor(gram):
    n = gram.shape[0]
    rows = lax.broadcasted_iota(jnp.int32, (n, 128), 0)
    lanes = lax.broadcasted_iota(jnp.int32, (n, 128), 1)
    unit = jnp.where(lanes == rows + n, 1.0, 0.0).astype(F32)
    work = jnp.concatenate([gram, jnp.zeros((n, 128 - n), F32)], axis=1) + unit
    for k in range(n):
        scale = lax.rsqrt(work[k : k + 1, k : k + 1])
        line = work[k : k + 1, :] * scale
        col = work[:, k : k + 1] * scale
        work = jnp.where(rows > k, work - col * line, jnp.where(rows == k, line, work))
    return work[:, n : 2 * n]


GROUPS = ((0, 512), (512, 384))


def kernel(
    tok_in, og_in, wu_in, wd_in, uq_in, dq_in, uacc, dacc,
    ig_out, ul_out, ur_out, dl_out, dr_out, mu_out, md_out,
    TO, ACT, UQ, DQ, AU, AD, GQ, UL, UR, DL, DR,
    A, WU, WD, WIN, PF, SB, FB, RB, HG, IGP, IGX, PS, RY, FY, IGO, MU, MD,
    P28, R28, L28, P8, R8T, R8D, L8, GR,
    in_sem, acc_sem, out_sem, ring_s, ring_r, xs, xr, ys, yr, ds, dr, ws, wr,
    rs_s, rs_r, hs, hr, ps_s, ps_r, ry_s, ry_r, fs, fr, cs, cr, gs, gr,
):
    dp, t = lax.axis_index("dp"), lax.axis_index("tensor")
    z, x = dp // NX, lax.rem(dp, NX)
    y, c = t // 2, lax.rem(t, 2)
    mine = x // 2 == c
    xl, xrr = wrap(x - 1, NX), wrap(x + 1, NX)
    sib = (dp, t + 1 - 2 * c)
    tok, og = TO.at[0], TO.at[1]
    tokens = TO.shape[1]
    grad_scale = 1.0 / math.sqrt(tokens)

    def lanes_of(i):
        return pl.ds(pl.multiple_of(i * 128, 128), 128)

    def rcopy(src, dst, s, r, dev):
        return pltpu.make_async_remote_copy(
            src_ref=src, dst_ref=dst, send_sem=s, recv_sem=r, device_id=dev, device_id_type=MESH
        )

    def drain(ref, sem):
        pltpu.make_async_copy(ref, ref, sem).wait()

    def at_x(xi):
        return (z * NX + xi, t)

    loads = [
        pltpu.make_async_copy(src, dst, in_sem.at[i])
        for i, (src, dst) in enumerate(
            (
                (wu_in, WU.at[z]),
                (wd_in, WD.at[:, lanes_of(z)]),
                (tok_in, tok),
                (og_in, og),
                (uq_in, UQ),
                (dq_in, DQ),
            )
        )
    ]
    load_u = pltpu.make_async_copy(uacc.at[0], MU, acc_sem.at[0])
    load_d = pltpu.make_async_copy(dacc.at[0], MD, acc_sem.at[1])
    for load in loads:
        load.start()
    load_u.start()
    load_d.start()

    barrier = pltpu.get_barrier_semaphore()

    def greet_dp(j, carry):
        @pl.when(j != dp)
        def _():
            pl.semaphore_signal(barrier, inc=1, device_id=(j, t), device_id_type=MESH)

        return carry

    def greet_t(j, carry):
        @pl.when(j != t)
        def _():
            pl.semaphore_signal(barrier, inc=1, device_id=(dp, j), device_id_type=MESH)

        return carry

    lax.fori_loop(0, NDP, greet_dp, 0)
    lax.fori_loop(0, NT, greet_t, 0)

    @pl.when(jnp.logical_not(mine))
    def _():
        for h in range(2):
            pl.semaphore_signal(
                barrier,
                inc=1,
                device_id=(z * NX + 2 * c + h, 2 * y + x // 2),
                device_id_type=MESH,
            )

    pl.semaphore_wait(barrier, NDP + NT - 2 + 2 * jnp.where(mine, 0, 1).astype(jnp.int32))

    for load in loads[:4]:
        load.wait()
    for h in range(2):

        @pl.when(jnp.logical_and(mine, lax.rem(x, 2) == h))
        def _():
            for arr in range(2):
                A[arr, x, :, lanes_of(y)] = TO[arr, :, h * 128 : (h + 1) * 128]

    @pl.when(t == 0)
    def _():
        WIN[...] = TO[...]

    def slot(mat, zi, g):
        hidden_range = pl.ds(*GROUPS[g])
        if mat == 0:
            return WU.at[zi, :, hidden_range]
        return WD.at[hidden_range, lanes_of(zi)]

    def ring(mat, way, step, g):
        if way == 0:
            zi, to = wrap(z - step + 1, NZ), wrap(z + 1, NZ)
        else:
            zi, to = wrap(z + step - 1, NZ), wrap(z - 1, NZ)
        i = (mat, way, g, step - 1)
        ref = slot(mat, zi, g)
        return rcopy(ref, ref, ring_s.at[i], ring_r.at[i], (to * NX + x, t))

    def ring_ways(step, g):
        return (0, 1) if step < 4 else (g,)

    def ring_send(mat, step, g):
        for way in ring_ways(step, g):
            ring(mat, way, step, g).start()

    def ring_arrived(mat, way, step, g):
        zi = wrap(z - step, NZ) if way == 0 else wrap(z + step, NZ)
        ref = slot(mat, zi, g)
        i = (mat, way, g, step - 1)
        rcopy(ref, ref, ring_s.at[i], ring_r.at[i], (dp, t)).wait_recv()

    def ring_pass(mat, step, g):
        for way in ring_ways(step - 1, g):
            ring_arrived(mat, way, step - 1, g)
            if way in ring_ways(step, g):
                ring(mat, way, step, g).start()

    def ring_end(mat, g):
        for way in ring_ways(4, g):
            ring_arrived(mat, way, 4, g)

    ring_send(0, 1, 0)
    ring_send(1, 1, 0)

    def piece(arr, h):
        xd = 2 * c + h
        src = TO.at[arr, :, pl.ds(h * 128, 128)]
        return rcopy(
            src,
            A.at[arr, x, :, lanes_of(y)],
            xs.at[arr, h],
            xr.at[arr, lax.rem(x, 2)],
            (z * NX + xd, 2 * y + x // 2),
        )

    def foreign(h):
        return jnp.logical_not(jnp.logical_and(mine, lax.rem(x, 2) == h))

    for arr in range(2):
        for h in range(2):

            @pl.when(foreign(h))
            def _():
                piece(arr, h).start()

    def pair(arr, yi):
        return A.at[arr, pl.ds(2 * c, 2), :, lanes_of(yi)]

    def spread(arr, off):
        yd = wrap(y + off, NY)
        return rcopy(pair(arr, y), pair(arr, y), ys.at[arr, off], yr.at[arr, off], (dp, 2 * yd + c))

    def to_sibling(arr, yi, off):
        return rcopy(pair(arr, yi), pair(arr, yi), ds.at[arr, off], dr.at[arr, off], sib)

    for arr in range(2):
        for h in range(2):

            @pl.when(foreign(h))
            def _():
                ref = A.at[arr, 2 * c + h, :, lanes_of(y)]
                rcopy(ref, ref, xs.at[arr, h], xr.at[arr, h], (dp, t)).wait_recv()

        for off in (4, 3, 5, 2, 6, 1, 7):
            spread(arr, off).start()
        to_sibling(arr, y, 0).start()

    @pl.when(t == 0)
    def _():
        def one(j, carry):
            rcopy(tok, WIN.at[0], ws.at[0], wr.at[0], (dp, j)).start()
            rcopy(og, WIN.at[1], ws.at[1], wr.at[1], (dp, j)).start()
            return carry

        lax.fori_loop(1, NT, one, 0)

    def y_arrivals(arr):
        for off in (1, 7, 2, 6, 3, 5, 4):
            yi = wrap(y - off, NY)
            ref = pair(arr, yi)
            rcopy(ref, ref, ys.at[arr, off], yr.at[arr, off], (dp, t)).wait_recv()
            to_sibling(arr, yi, off).start()

    def sibling_arrivals(arr):
        for off in range(NY):
            yi = wrap(y - off, NY)
            ref = A.at[arr, pl.ds(2 - 2 * c, 2), :, lanes_of(yi)]
            rcopy(ref, ref, ds.at[arr, off], dr.at[arr, off], (dp, t)).wait_recv()

    def products(mat, g):
        lo, size = GROUPS[g]
        cols = slice(lo, lo + size)

        def one(d, carry):
            xi = wrap(x + d, NX)
            if mat == 0:
                PF[0, d, :, cols] = dot_nn(A[0, xi], WU[:, :, cols].reshape(NZ * 128, size))
            else:
                PF[1, d, :, cols] = dot_nt(A[1, xi], WD[cols, :])
            return carry

        lax.fori_loop(0, NX, one, 0)

    half_rows = tokens // 2
    top, bot = pl.ds(0, half_rows), pl.ds(half_rows, half_rows)

    def rs_copy(mat, g, i):
        cols = pl.ds(*GROUPS[g])
        src = (SB.at[mat, 1, top, cols], SB.at[mat, 1, bot, cols], SB.at[mat, 0, bot, cols],
               SB.at[mat, 2, top, cols], SB.at[mat, 0, top, cols], SB.at[mat, 2, bot, cols])[i]
        dst = (FB.at[mat, 0, :, cols], FB.at[mat, 1, :, cols], RB.at[mat, 0, bot, cols],
               RB.at[mat, 1, top, cols], RB.at[mat, 0, top, cols], RB.at[mat, 1, bot, cols])[i]
        to = at_x(xrr if i % 2 == 0 else xl)
        return rcopy(src, dst, rs_s.at[mat, g, i], rs_r.at[mat, g, i], to)

    def rs_first(mat, g):
        cols = slice(GROUPS[g][0], sum(GROUPS[g]))
        SB[mat, 1, :, cols] = PF[mat, 2, :, cols].astype(BF16)
        rs_copy(mat, g, 0).start()
        rs_copy(mat, g, 1).start()
        SB[mat, 0, half_rows:, cols] = PF[mat, 1, half_rows:, cols].astype(BF16)
        rs_copy(mat, g, 2).start()
        SB[mat, 2, :half_rows, cols] = PF[mat, 3, :half_rows, cols].astype(BF16)
        rs_copy(mat, g, 3).start()

    def rs_second(mat, g):
        cols = slice(GROUPS[g][0], sum(GROUPS[g]))
        rs_copy(mat, g, 0).wait_recv()
        SB[mat, 0, :half_rows, cols] = (
            PF[mat, 1, :half_rows, cols] + FB[mat, 0, :, cols].astype(F32)
        ).astype(BF16)
        rs_copy(mat, g, 4).start()
        rs_copy(mat, g, 1).wait_recv()
        SB[mat, 2, half_rows:, cols] = (
            PF[mat, 3, half_rows:, cols] + FB[mat, 1, :, cols].astype(F32)
        ).astype(BF16)
        rs_copy(mat, g, 5).start()

    def rs_end(mat, g):
        for i in range(2, 6):
            rs_copy(mat, g, i).wait_recv()

    ring_pass(0, 2, 0)
    ring_pass(1, 2, 0)
    loads[4].wait()
    load_u.wait()
    AU[...] = dot_nt(UQ[...], MU[...], HI)
    ring_pass(0, 3, 0)
    ring_pass(1, 3, 0)
    ring_send(0, 1, 1)
    loads[5].wait()
    load_d.wait()
    AD[...] = dot_nt(DQ[...], MD[...], HI)
    ring_pass(0, 4, 0)
    ring_pass(1, 4, 0)
    ring_send(1, 1, 1)
    y_arrivals(0)
    ring_pass(0, 2, 1)
    ring_end(0, 0)
    sibling_arrivals(0)
    products(0, 0)
    rs_first(0, 0)
    ring_pass(1, 2, 1)
    y_arrivals(1)
    ring_pass(0, 3, 1)
    ring_end(1, 0)
    sibling_arrivals(1)
    products(1, 0)
    rs_first(1, 0)
    rs_second(0, 0)
    ring_pass(1, 3, 1)
    ring_pass(0, 4, 1)
    ring_pass(1, 4, 1)

    @pl.when(t != 0)
    def _():
        for arr in range(2):
            rcopy(WIN.at[arr], WIN.at[arr], ws.at[arr], wr.at[arr], (dp, t)).wait_recv()

    GQ[...] = dot_nt(DQ[...], WIN[1].astype(F32), HI)
    rs_second(1, 0)

    def activate(g):
        cols = slice(GROUPS[g][0], sum(GROUPS[g]))
        preact = PF[0, 0, :, cols] + RB[0, 0, :, cols].astype(F32) + RB[0, 1, :, cols].astype(F32)
        back = PF[1, 0, :, cols] + RB[1, 0, :, cols].astype(F32) + RB[1, 1, :, cols].astype(F32)
        squash = jax.nn.sigmoid(preact)
        ACT[:, cols] = (preact * squash).astype(BF16)
        HG[x, :, cols] = (back * squash * (1.0 + preact * (1.0 - squash))).astype(BF16)

    def add_up(g):
        cols = slice(GROUPS[g][0], sum(GROUPS[g]))
        hq = dot_nt(UQ[:, cols], HG[x, :, cols].astype(F32), HI)
        AU[...] += dot_nn(hq, WIN[0].astype(F32), HI) * grad_scale

    def add_down(g):
        cols = slice(GROUPS[g][0], sum(GROUPS[g]))
        AD[:, cols] += dot_nn(GQ[...], ACT[:, cols].astype(F32), HI) * grad_scale

    def h_copy(g, i):
        cols = pl.ds(*GROUPS[g])
        own = HG.at[x, :, cols]
        src = (own, own, HG.at[xl, top, cols], HG.at[xrr, bot, cols])[i]
        return rcopy(src, src, hs.at[g, i], hr.at[g, i], at_x(xrr if i % 2 == 0 else xl))

    def h_wait(g, i):
        cols = pl.ds(*GROUPS[g])
        x2 = wrap(x + 2, NX)
        ref = (
            HG.at[xl, :, cols], HG.at[xrr, :, cols], HG.at[x2, top, cols], HG.at[x2, bot, cols]
        )[i]
        rcopy(ref, ref, hs.at[g, i], hr.at[g, i], (dp, t)).wait_recv()

    def h_relay(g):
        h_wait(g, 0)
        h_copy(g, 2).start()
        h_wait(g, 1)
        h_copy(g, 3).start()

    ring_end(0, 1)
    products(0, 1)
    rs_first(0, 1)
    ring_end(1, 1)
    products(1, 1)
    rs_first(1, 1)
    rs_second(0, 1)
    rs_second(1, 1)
    rs_end(0, 0)
    rs_end(1, 0)
    activate(0)
    h_copy(0, 0).start()
    h_copy(0, 1).start()
    add_up(0)
    add_down(0)
    rs_end(0, 1)
    rs_end(1, 1)
    activate(1)

    def along(at, n, visit, here):
        visit(wrap(at + n // 2, n))

        def one(i, carry):
            visit(wrap(at + n // 2 - i, n))
            visit(wrap(at + n // 2 + i, n))
            return carry

        lax.fori_loop(1, n // 2, one, 0)
        here()

    other_x = [wrap(x + d, NX) for d in (2, 1, 3)]

    def dp_others(send):
        def visit(zi):
            for xi in (*other_x, x):
                send(zi * NX + xi)

        def here():
            for xi in other_x:
                send(z * NX + xi)

        along(z, NZ, visit, here)

    def t_others(send):
        def visit(yi):
            send(2 * yi)
            send(2 * yi + 1)

        along(y, NY, visit, lambda: send(2 * y + 1 - c))

    def put28(k, arr):
        for g in range(4):
            for l in range(7):
                P28[k, g * 7 + l] = arr[8 * g : 8 * g + 8, 128 * l : 128 * l + 128]

    def put8(k, arr):
        for g in range(4):
            for l in range(2):
                P8[k, g * 2 + l] = arr[8 * g : 8 * g + 8, 128 * l : 128 * l + 128]

    def get(buf, k, n):
        return jnp.concatenate(
            [jnp.concatenate([buf[k, g * n + l] for l in range(n)], axis=1) for g in range(4)],
            axis=0,
        )

    def send28(k):
        def one(j):
            @pl.when(j < 28)
            def _():
                rcopy(P28.at[k, j], R28.at[k, dp], cs.at[k, 0], cr.at[k, 0], (j, t)).start()

        dp_others(one)

        @pl.when(dp < 28)
        def _():
            R28[k, dp] = P28[k, dp]

    def reduce28(k):
        @pl.when(dp < 28)
        def _():
            drain(R28.at[k, pl.ds(0, 31)], cr.at[k, 0])
            L28[k, dp] = jnp.sum(R28[k], axis=0)

            def one(j):
                rcopy(L28.at[k, dp], L28.at[k, dp], cs.at[k, 1], cr.at[k, 1], (j, t)).start()

            dp_others(one)

    def end28(k):
        @pl.when(dp < 28)
        def _():
            drain(L28.at[k, pl.ds(0, 27)], cr.at[k, 1])

        @pl.when(dp >= 28)
        def _():
            drain(L28.at[k, pl.ds(0, 28)], cr.at[k, 1])

    def send8(k):
        def one(j, carry):
            @pl.when(j != t)
            def _():
                rcopy(P8.at[k, j], R8T.at[k, t], cs.at[k, 2], cr.at[k, 2], (dp, j)).start()

            return carry

        lax.fori_loop(0, 8, one, 0)

        @pl.when(t < 8)
        def _():
            R8T[k, t] = P8[k, t]

    def middle8(k):
        @pl.when(t < 8)
        def _():
            drain(R8T.at[k, pl.ds(0, 15)], cr.at[k, 2])
            R8D[k, dp] = jnp.sum(R8T[k], axis=0)

            def one(j):
                rcopy(R8D.at[k, dp], R8D.at[k, dp], cs.at[k, 3], cr.at[k, 3], (j, t)).start()

            dp_others(one)

    def reduce8(k):
        @pl.when(t < 8)
        def _():
            drain(R8D.at[k, pl.ds(0, 31)], cr.at[k, 3])
            L8[k, t] = jnp.sum(R8D[k], axis=0)

            def one(j):
                rcopy(L8.at[k, t], L8.at[k, t], cs.at[k, 4], cr.at[k, 4], (dp, j)).start()

            t_others(one)

    def end8(k):
        @pl.when(t < 8)
        def _():
            drain(L8.at[k, pl.ds(0, 7)], cr.at[k, 4])

        @pl.when(t >= 8)
        def _():
            drain(L8.at[k, pl.ds(0, 8)], cr.at[k, 4])

    add_up(1)
    put8(0, AU[...])
    send8(0)
    add_down(1)
    put28(0, AD[...])
    send28(0)

    def ig_product(i):
        IGP[i] = dot_nt(HG[i], WU[...].reshape(NZ * 128, WU.shape[2])).astype(BF16)

    h_copy(1, 0).start()
    h_copy(1, 1).start()
    MU[...] += dot_nn(WIN[0].T, HG[x]) * grad_scale
    MD[...] += dot_nn(ACT[...].T, WIN[1]) * grad_scale
    store_u = pltpu.make_async_copy(MU, mu_out, acc_sem.at[0])
    store_d = pltpu.make_async_copy(MD, md_out, acc_sem.at[1])
    store_u.start()
    store_d.start()
    for mat in range(2):
        for g in range(2):
            for step in range(1, 5):
                for way in ring_ways(step, g):
                    ring(mat, way, step, g).wait_send()
            for i in range(6):
                rs_copy(mat, g, i).wait_send()
    for arr in range(2):
        for h in range(2):

            @pl.when(foreign(h))
            def _():
                piece(arr, h).wait_send()

        for off in range(1, NY):
            spread(arr, off).wait_send()
        for off in range(NY):
            to_sibling(arr, wrap(y - off, NY), off).wait_send()

    @pl.when(t == 0)
    def _():
        for arr in range(2):

            def one(j, carry):
                rcopy(WIN.at[arr], WIN.at[arr], ws.at[arr], wr.at[arr], (dp, j)).wait_send()
                return carry

            lax.fori_loop(1, NT, one, 0)

    h_relay(0)
    middle8(0)
    reduce28(0)
    h_relay(1)

    def ig_near(d, carry):
        ig_product(wrap(x + d - 1, NX))
        return carry

    lax.fori_loop(0, 3, ig_near, 0)
    reduce8(0)
    for g in range(2):
        h_wait(g, 2)
        h_wait(g, 3)
    lax.fori_loop(3, 4, ig_near, 0)
    other = IGP.at[pl.ds(2 - 2 * c, 2)]
    pair_copy = rcopy(other, IGX, ps_s.at[0], ps_r.at[0], sib)
    pair_copy.start()

    end28(0)
    down_sum = get(L28, 0, 7)
    put8(1, dot_nn(down_sum, MD[...], HI))
    send8(1)
    gram_part = dot_nt(down_sum, down_sum, HI)
    GR[t] = jnp.concatenate([gram_part[8 * g : 8 * g + 8] for g in range(4)], axis=1)

    def gram_send(j):
        rcopy(GR.at[t], GR.at[t], gs.at[0], gr.at[0], (dp, j)).start()

    t_others(gram_send)

    pair_copy.wait_recv()
    for i in range(2):
        both = (IGP[2 * c + i].astype(F32) + IGX[i].astype(F32)).astype(BF16)
        for k in range(NY):
            PS[k, i] = both[:, k * 128 : (k + 1) * 128]
    RY[y] = PS[y]

    def ry_send(j):
        rcopy(PS.at[j], RY.at[y], ry_s.at[0], ry_r.at[0], (dp, 2 * j + c)).start()

    along(y, NY, ry_send, lambda: None)

    end8(0)
    up_sum = get(L8, 0, 2)
    put28(1, dot_nn(up_sum, MU[...], HI))
    send28(1)
    middle8(1)

    def sums_left(k):
        @pl.when(dp < 28)
        def _():
            drain(P28.at[k, pl.ds(0, 27)], cs.at[k, 0])
            drain(R28.at[k, pl.ds(0, 31)], cs.at[k, 1])

        @pl.when(dp >= 28)
        def _():
            drain(P28.at[k, pl.ds(0, 28)], cs.at[k, 0])

        @pl.when(t < 8)
        def _():
            drain(P8.at[k, pl.ds(0, 7)], cs.at[k, 2])
            drain(R8D.at[k, pl.ds(0, 31)], cs.at[k, 3])
            drain(R8T.at[k, pl.ds(0, 15)], cs.at[k, 4])

        @pl.when(t >= 8)
        def _():
            drain(P8.at[k, pl.ds(0, 8)], cs.at[k, 2])

    def put_out(ref, value, dst, i):
        ref[...] = value
        copy = pltpu.make_async_copy(ref, dst, out_sem.at[i])
        copy.start()
        return copy

    results = []
    up_inv = inverse_factor(dot_nt(up_sum, up_sum, HI))
    results.append(put_out(UL, dot_nn(up_inv, up_sum, HI), ul_out, 0))
    store_u.wait()
    store_d.wait()
    sums_left(0)
    for g in range(2):
        for i in range(4):
            h_copy(g, i).wait_send()
    pair_copy.wait_send()
    reduce28(1)
    drain(GR.at[pl.ds(0, NT - 1)], gr.at[0])
    packed = jnp.sum(GR[...], axis=0)
    gram = jnp.concatenate([packed[:, 32 * g : 32 * g + 32] for g in range(4)], axis=0)
    reduce8(1)
    down_inv = inverse_factor(gram)
    results.append(put_out(DL, dot_nn(down_inv, down_sum, HI), dl_out, 1))

    drain(RY.at[pl.ds(0, NY - 1)], ry_r.at[0])
    for i in range(2):
        FY[i] = jnp.sum(RY[:, i].astype(F32), axis=0).astype(BF16)

    def last(i, h):
        return rcopy(
            FY.at[i],
            IGO.at[h],
            fs.at[i],
            fr.at[h],
            (z * NX + 2 * c + i, 2 * y + x // 2),
        )

    for h in range(2):
        for i in range(2):

            @pl.when(jnp.logical_and(lax.rem(x, 2) == h, foreign(i)))
            def _():
                last(i, h).start()

        @pl.when(jnp.logical_and(mine, lax.rem(x, 2) == h))
        def _():
            IGO[h] = FY[h]

    end28(1)
    results.append(
        put_out(UR, dot_nn(up_inv, get(L28, 1, 7), HI) * (1.0 / NDP), ur_out, 2)
    )
    for h in range(2):

        @pl.when(foreign(h))
        def _():
            rcopy(IGO.at[h], IGO.at[h], fs.at[h], fr.at[h], (dp, t)).wait_recv()

        copy = pltpu.make_async_copy(
            IGO.at[h], ig_out.at[:, pl.ds(h * 128, 128)], out_sem.at[4 + h]
        )
        copy.start()
        results.append(copy)
    end8(1)
    results.append(
        put_out(DR, dot_nn(down_inv, get(L8, 1, 2), HI) * (1.0 / NDP), dr_out, 3)
    )

    drain(PS.at[pl.ds(0, NY - 1)], ry_s.at[0])
    for i in range(2):

        @pl.when(foreign(i))
        def _():
            rcopy(FY.at[i], FY.at[i], fs.at[i], fr.at[i], (dp, t)).wait_send()

    sums_left(1)
    drain(GR.at[pl.ds(0, NT - 1)], gs.at[0])
    for copy in results:
        copy.wait()


def finish(*refs):
    ins, outs, held = refs[:7], refs[7:14], refs[14:21]
    came, left = refs[21], refs[22]
    loads = [pltpu.make_async_copy(ins[i], held[i], came.at[i]) for i in range(7)]
    ends = [outs[i] if i < 5 else outs[i].at[0] for i in range(7)]
    stores = [pltpu.make_async_copy(held[i], ends[i], left.at[i]) for i in range(7)]
    for i in (1, 2, 5, 3, 4, 6, 0):
        loads[i].start()
    for i, low, high in ((5, 1, 2), (6, 3, 4)):
        for k in (low, high, i):
            loads[k].wait()
        held[i][...] -= dot_thirds(held[low][...], held[high][...])
        for k in (i, low, high):
            stores[k].start()
    loads[0].wait()
    stores[0].start()
    for store in stores:
        store.wait()


def shards(tokens, out_grad, up_weight, down_weight, up_accum, down_accum, up_q, down_q):
    rows, feats = tokens.shape
    hid = up_weight.shape[1]
    win = up_accum.shape[1]
    rank = up_q.shape[1]
    quarter = NZ * 128
    hbm = pl.BlockSpec(memory_space=pl.ANY)
    sem = pltpu.SemaphoreType.DMA
    V = pltpu.VMEM
    shape = jax.ShapeDtypeStruct
    outs = pl.pallas_call(
        kernel,
        out_shape=[
            shape((rows, feats), BF16),
            shape((rank, win), F32),
            shape((rank, hid), F32),
            shape((rank, hid), F32),
            shape((rank, win), F32),
            shape((win, hid), F32),
            shape((hid, win), F32),
        ],
        in_specs=[hbm] * 8,
        out_specs=[hbm] * 7,
        scratch_shapes=[
            V((2, rows, feats), BF16),
            V((rows, hid), BF16),
            V((rank, hid), F32),
            V((rank, win), F32),
            V((rank, win), F32),
            V((rank, hid), F32),
            V((rank, rows), F32),
            V((rank, win), F32),
            V((rank, hid), F32),
            V((rank, hid), F32),
            V((rank, win), F32),
            V((2, NX, rows, quarter), BF16),
            V((NZ, 128, hid), BF16),
            V((hid, quarter), BF16),
            V((2, rows, win), BF16),
            V((2, NX, rows, hid), F32),
            V((2, 3, rows, hid), BF16),
            V((2, 2, rows // 2, hid), BF16),
            V((2, 2, rows, hid), BF16),
            V((NX, rows, hid), BF16),
            V((NX, rows, quarter), BF16),
            V((2, rows, quarter), BF16),
            V((NY, 2, rows, 128), BF16),
            V((NY, 2, rows, 128), BF16),
            V((2, rows, 128), BF16),
            V((2, rows, 128), BF16),
            V((win, hid), F32),
            V((hid, win), F32),
            V((2, 28, 8, 128), F32),
            V((2, NDP, 8, 128), F32),
            V((2, 28, 8, 128), F32),
            V((2, 8, 8, 128), F32),
            V((2, NT, 8, 128), F32),
            V((2, NDP, 8, 128), F32),
            V((2, 8, 8, 128), F32),
            V((NT, 8, 128), F32),
            sem((6,)),
            sem((2,)),
            sem((6,)),
            sem((2, 2, 2, 4)),
            sem((2, 2, 2, 4)),
            sem((2, 2)),
            sem((2, 2)),
            sem((2, NY)),
            sem((2, NY)),
            sem((2, NY)),
            sem((2, NY)),
            sem((2,)),
            sem((2,)),
            sem((2, 2, 6)),
            sem((2, 2, 6)),
            sem((2, 4)),
            sem((2, 4)),
            sem((1,)),
            sem((1,)),
            sem((1,)),
            sem((1,)),
            sem((2,)),
            sem((2,)),
            sem((2, 5)),
            sem((2, 5)),
            sem((1,)),
            sem((1,)),
        ],
        compiler_params=pltpu.CompilerParams(
            collective_id=0, has_side_effects=True, vmem_limit_bytes=63 * 1024 * 1024
        ),
    )(tokens, out_grad, up_weight, down_weight, up_q.T, down_q.T, up_accum, down_accum)
    input_grad, ul, ur, dl, dr, mu, md = outs
    results = pl.pallas_call(
        finish,
        out_shape=[
            shape((rows, feats), BF16),
            shape((rank, win), F32),
            shape((rank, hid), F32),
            shape((rank, hid), F32),
            shape((rank, win), F32),
            shape(up_accum.shape, F32),
            shape(down_accum.shape, F32),
        ],
        in_specs=[hbm] * 7,
        out_specs=[hbm] * 7,
        scratch_shapes=[
            V((rows, feats), BF16),
            V((rank, win), F32),
            V((rank, hid), F32),
            V((rank, hid), F32),
            V((rank, win), F32),
            V((win, hid), F32),
            V((hid, win), F32),
            sem((7,)),
            sem((7,)),
        ],
        compiler_params=pltpu.CompilerParams(vmem_limit_bytes=63 * 1024 * 1024),
    )(input_grad, ul, ur, dl, dr, mu, md)
    input_grad, ul, ur, dl, dr, up_error, down_error = results
    return input_grad, up_error, ul.T, ur.T, down_error, dl.T, dr.T


def solution(mesh):
    return jax.shard_map(
        shards,
        mesh=mesh,
        in_specs=(
            P("dp", "tensor"),
            P("dp", "tensor"),
            P("dp", "tensor"),
            P("tensor", "dp"),
            P("dp", None, "tensor"),
            P("dp", "tensor", None),
            P("tensor", None),
            P(),
        ),
        out_specs=(
            P("dp", "tensor"),
            P("dp", None, "tensor"),
            P(),
            P("tensor", None),
            P("dp", "tensor", None),
            P("tensor", None),
            P(),
        ),
        check_vma=False,
    )
```

```python
import functools
import math

import jax
import jax.numpy as jnp
from jax import lax
from jax.experimental import pallas as pl
from jax.experimental.pallas import tpu as pltpu
from jax.sharding import PartitionSpec as P

MESH = pl.DeviceIdType.MESH
HI = lax.Precision.HIGHEST
NZ, NX, NY = 8, 4, 8
NDP, NT = 32, 16
F32, BF16 = jnp.float32, jnp.bfloat16


def wrap(a, n):
    return lax.rem(a + 4 * n, n)


def thirds(a):
    high = a.astype(BF16)
    rest = a - high.astype(F32)
    middle = rest.astype(BF16)
    return high, middle, (rest - middle.astype(F32)).astype(BF16)


def dot_thirds(left_t, right_t):
    lh, lm, ll = thirds(left_t)
    rh, rm, rl = thirds(right_t)
    left = jnp.concatenate([ll, lm, lh, lm, lh, lh], axis=0)
    right = jnp.concatenate([rh, rm, rl, rh, rm, rh], axis=0)
    return dot_nn(left.astype(F32).T.astype(BF16), right)


def dot_nt(a, b, precision=None):
    return lax.dot_general(
        a, b, (((1,), (1,)), ((), ())), preferred_element_type=F32, precision=precision
    )


def dot_nn(a, b, precision=None):
    return jnp.dot(a, b, preferred_element_type=F32, precision=precision)


def inverse_factor(gram):
    n = gram.shape[0]
    rows = lax.broadcasted_iota(jnp.int32, (n, 128), 0)
    lanes = lax.broadcasted_iota(jnp.int32, (n, 128), 1)
    unit = jnp.where(lanes == rows + n, 1.0, 0.0).astype(F32)
    work = jnp.concatenate([gram, jnp.zeros((n, 128 - n), F32)], axis=1) + unit
    for k in range(n):
        scale = lax.rsqrt(work[k : k + 1, k : k + 1])
        line = work[k : k + 1, :] * scale
        col = work[:, k : k + 1] * scale
        work = jnp.where(rows > k, work - col * line, jnp.where(rows == k, line, work))
    return work[:, n : 2 * n]


GROUPS = ((0, 512), (512, 384))


def kernel(
    tok_in, og_in, wu_in, wd_in, uq_in, dq_in, uacc, dacc,
    ig_out, ul_out, ur_out, dl_out, dr_out, mu_out, md_out,
    TO, ACT, UQ, DQ, AU, AD, GQ, UL, UR, DL, DR,
    A, WU, WD, WIN, PF, SB, FB, RB, HG, IGP, IGX, PS, RY, FY, IGO, MU, MD,
    P28, R28, L28, P8, R8T, R8D, L8, GR,
    in_sem, acc_sem, out_sem, ring_s, ring_r, xs, xr, ys, yr, ds, dr, ws, wr,
    rs_s, rs_r, hs, hr, ps_s, ps_r, ry_s, ry_r, fs, fr, cs, cr, gs, gr,
):
    dp, t = lax.axis_index("dp"), lax.axis_index("tensor")
    z, x = dp // NX, lax.rem(dp, NX)
    y, c = t // 2, lax.rem(t, 2)
    mine = x // 2 == c
    xl, xrr = wrap(x - 1, NX), wrap(x + 1, NX)
    sib = (dp, t + 1 - 2 * c)
    tok, og = TO.at[0], TO.at[1]
    tokens = TO.shape[1]
    grad_scale = 1.0 / math.sqrt(tokens)

    def lanes_of(i):
        return pl.ds(pl.multiple_of(i * 128, 128), 128)

    def rcopy(src, dst, s, r, dev):
        return pltpu.make_async_remote_copy(
            src_ref=src, dst_ref=dst, send_sem=s, recv_sem=r, device_id=dev, device_id_type=MESH
        )

    def drain(ref, sem):
        pltpu.make_async_copy(ref, ref, sem).wait()

    def at_x(xi):
        return (z * NX + xi, t)

    loads = [
        pltpu.make_async_copy(src, dst, in_sem.at[i])
        for i, (src, dst) in enumerate(
            (
                (wu_in, WU.at[z]),
                (wd_in, WD.at[:, lanes_of(z)]),
                (tok_in, tok),
                (og_in, og),
                (uq_in, UQ),
                (dq_in, DQ),
            )
        )
    ]
    load_u = pltpu.make_async_copy(uacc.at[0], MU, acc_sem.at[0])
    load_d = pltpu.make_async_copy(dacc.at[0], MD, acc_sem.at[1])
    for load in loads:
        load.start()
    load_u.start()
    load_d.start()

    barrier = pltpu.get_barrier_semaphore()

    def greet_dp(j, carry):
        @pl.when(j != dp)
        def _():
            pl.semaphore_signal(barrier, inc=1, device_id=(j, t), device_id_type=MESH)

        return carry

    def greet_t(j, carry):
        @pl.when(j != t)
        def _():
            pl.semaphore_signal(barrier, inc=1, device_id=(dp, j), device_id_type=MESH)

        return carry

    lax.fori_loop(0, NDP, greet_dp, 0)
    lax.fori_loop(0, NT, greet_t, 0)

    @pl.when(jnp.logical_not(mine))
    def _():
        for h in range(2):
            pl.semaphore_signal(
                barrier,
                inc=1,
                device_id=(z * NX + 2 * c + h, 2 * y + x // 2),
                device_id_type=MESH,
            )

    for load in loads[:4]:
        load.wait()
    for h in range(2):

        @pl.when(jnp.logical_and(mine, lax.rem(x, 2) == h))
        def _():
            for arr in range(2):
                A[arr, x, :, lanes_of(y)] = TO[arr, :, h * 128 : (h + 1) * 128]

    @pl.when(t == 0)
    def _():
        WIN[...] = TO[...]

    pl.semaphore_wait(barrier, NDP + NT - 2 + 2 * jnp.where(mine, 0, 1).astype(jnp.int32))

    def slot(mat, zi, g):
        hidden_range = pl.ds(*GROUPS[g])
        if mat == 0:
            return WU.at[zi, :, hidden_range]
        return WD.at[hidden_range, lanes_of(zi)]

    def ring(mat, way, step, g):
        if way == 0:
            zi, to = wrap(z - step + 1, NZ), wrap(z + 1, NZ)
        else:
            zi, to = wrap(z + step - 1, NZ), wrap(z - 1, NZ)
        i = (mat, way, g, step - 1)
        ref = slot(mat, zi, g)
        return rcopy(ref, ref, ring_s.at[i], ring_r.at[i], (to * NX + x, t))

    def ring_ways(step, g):
        return (0, 1) if step < 4 else (g,)

    def ring_send(mat, step, g):
        for way in ring_ways(step, g):
            ring(mat, way, step, g).start()

    def ring_arrived(mat, way, step, g):
        zi = wrap(z - step, NZ) if way == 0 else wrap(z + step, NZ)
        ref = slot(mat, zi, g)
        i = (mat, way, g, step - 1)
        rcopy(ref, ref, ring_s.at[i], ring_r.at[i], (dp, t)).wait_recv()

    def ring_pass(mat, step, g):
        for way in ring_ways(step - 1, g):
            ring_arrived(mat, way, step - 1, g)
            if way in ring_ways(step, g):
                ring(mat, way, step, g).start()

    def ring_hop(mat, way, step, g):
        ring_arrived(mat, way, step - 1, g)
        ring(mat, way, step, g).start()

    def ring_end(mat, g):
        for way in ring_ways(4, g):
            ring_arrived(mat, way, 4, g)

    ring_send(0, 1, 0)
    ring_send(1, 1, 0)

    def piece(arr, h):
        xd = 2 * c + h
        src = TO.at[arr, :, pl.ds(h * 128, 128)]
        return rcopy(
            src,
            A.at[arr, x, :, lanes_of(y)],
            xs.at[arr, h],
            xr.at[arr, lax.rem(x, 2)],
            (z * NX + xd, 2 * y + x // 2),
        )

    def foreign(h):
        return jnp.logical_not(jnp.logical_and(mine, lax.rem(x, 2) == h))

    for arr in range(2):
        for h in range(2):

            @pl.when(foreign(h))
            def _():
                piece(arr, h).start()

    def pair(arr, yi):
        return A.at[arr, pl.ds(2 * c, 2), :, lanes_of(yi)]

    def spread(arr, off):
        yd = wrap(y + off, NY)
        return rcopy(pair(arr, y), pair(arr, y), ys.at[arr, off], yr.at[arr, off], (dp, 2 * yd + c))

    def to_sibling(arr, yi, off):
        return rcopy(pair(arr, yi), pair(arr, yi), ds.at[arr, off], dr.at[arr, off], sib)

    for arr in range(2):
        for h in range(2):

            @pl.when(foreign(h))
            def _():
                ref = A.at[arr, 2 * c + h, :, lanes_of(y)]
                rcopy(ref, ref, xs.at[arr, h], xr.at[arr, h], (dp, t)).wait_recv()

        for off in (4, 3, 5, 2, 6, 1, 7):
            spread(arr, off).start()
        to_sibling(arr, y, 0).start()

    @pl.when(t == 0)
    def _():
        def one(j, carry):
            rcopy(tok, WIN.at[0], ws.at[0], wr.at[0], (dp, j)).start()
            rcopy(og, WIN.at[1], ws.at[1], wr.at[1], (dp, j)).start()
            return carry

        lax.fori_loop(1, NT, one, 0)

    def y_arrivals(arr):
        for off in (1, 7, 2, 6, 3, 5, 4):
            yi = wrap(y - off, NY)
            ref = pair(arr, yi)
            rcopy(ref, ref, ys.at[arr, off], yr.at[arr, off], (dp, t)).wait_recv()
            to_sibling(arr, yi, off).start()

    def sibling_arrivals(arr):
        for off in range(NY):
            yi = wrap(y - off, NY)
            ref = A.at[arr, pl.ds(2 - 2 * c, 2), :, lanes_of(yi)]
            rcopy(ref, ref, ds.at[arr, off], dr.at[arr, off], (dp, t)).wait_recv()

    def products(mat, g):
        lo, size = GROUPS[g]
        cols = slice(lo, lo + size)

        def one(d, carry):
            xi = wrap(x + d, NX)
            if mat == 0:
                PF[0, d, :, cols] = dot_nn(A[0, xi], WU[:, :, cols].reshape(NZ * 128, size))
            else:
                PF[1, d, :, cols] = dot_nt(A[1, xi], WD[cols, :])
            return carry

        lax.fori_loop(0, NX, one, 0)

    half_rows = tokens // 2
    top, bot = pl.ds(0, half_rows), pl.ds(half_rows, half_rows)

    def rs_copy(mat, g, i):
        cols = pl.ds(*GROUPS[g])
        src = (SB.at[mat, 1, top, cols], SB.at[mat, 1, bot, cols], SB.at[mat, 0, bot, cols],
               SB.at[mat, 2, top, cols], SB.at[mat, 0, top, cols], SB.at[mat, 2, bot, cols])[i]
        dst = (FB.at[mat, 0, :, cols], FB.at[mat, 1, :, cols], RB.at[mat, 0, bot, cols],
               RB.at[mat, 1, top, cols], RB.at[mat, 0, top, cols], RB.at[mat, 1, bot, cols])[i]
        to = at_x(xrr if i % 2 == 0 else xl)
        return rcopy(src, dst, rs_s.at[mat, g, i], rs_r.at[mat, g, i], to)

    def rs_first(mat, g):
        cols = slice(GROUPS[g][0], sum(GROUPS[g]))
        SB[mat, 1, :, cols] = PF[mat, 2, :, cols].astype(BF16)
        rs_copy(mat, g, 0).start()
        rs_copy(mat, g, 1).start()
        SB[mat, 0, half_rows:, cols] = PF[mat, 1, half_rows:, cols].astype(BF16)
        rs_copy(mat, g, 2).start()
        SB[mat, 2, :half_rows, cols] = PF[mat, 3, :half_rows, cols].astype(BF16)
        rs_copy(mat, g, 3).start()

    def rs_second(mat, g):
        cols = slice(GROUPS[g][0], sum(GROUPS[g]))
        rs_copy(mat, g, 0).wait_recv()
        SB[mat, 0, :half_rows, cols] = (
            PF[mat, 1, :half_rows, cols] + FB[mat, 0, :, cols].astype(F32)
        ).astype(BF16)
        rs_copy(mat, g, 4).start()
        rs_copy(mat, g, 1).wait_recv()
        SB[mat, 2, half_rows:, cols] = (
            PF[mat, 3, half_rows:, cols] + FB[mat, 1, :, cols].astype(F32)
        ).astype(BF16)
        rs_copy(mat, g, 5).start()

    def rs_end(mat, g):
        for i in range(2, 6):
            rs_copy(mat, g, i).wait_recv()

    ring_pass(0, 2, 0)
    ring_pass(1, 2, 0)
    loads[4].wait()
    load_u.wait()
    AU[...] = dot_nt(UQ[...], MU[...], HI)
    ring_pass(0, 3, 0)
    ring_pass(1, 3, 0)
    for mat in range(2):
        ring(mat, 1, 1, 1).start()
    loads[5].wait()
    load_d.wait()
    AD[...] = dot_nt(DQ[...], MD[...], HI)
    for mat in range(2):
        ring_hop(mat, 0, 4, 0)
    for mat in range(2):
        ring_arrived(mat, 1, 3, 0)
    for mat in range(2):
        ring(mat, 0, 1, 1).start()
    y_arrivals(0)
    for mat in range(2):
        ring_hop(mat, 1, 2, 1)
    ring_end(0, 0)
    sibling_arrivals(0)
    products(0, 0)
    rs_first(0, 0)
    ring_hop(0, 1, 3, 1)
    ring_end(1, 0)
    ring_hop(1, 1, 3, 1)
    for mat in range(2):
        ring_hop(mat, 0, 2, 1)
    y_arrivals(1)
    sibling_arrivals(1)
    products(1, 0)
    rs_first(1, 0)
    rs_second(0, 0)
    for mat in range(2):
        ring_hop(mat, 1, 4, 1)
    for mat in range(2):
        ring_hop(mat, 0, 3, 1)

    @pl.when(t != 0)
    def _():
        for arr in range(2):
            rcopy(WIN.at[arr], WIN.at[arr], ws.at[arr], wr.at[arr], (dp, t)).wait_recv()

    GQ[...] = dot_nt(DQ[...], WIN[1].astype(F32), HI)
    rs_second(1, 0)

    def activate(g):
        cols = slice(GROUPS[g][0], sum(GROUPS[g]))
        preact = PF[0, 0, :, cols] + RB[0, 0, :, cols].astype(F32) + RB[0, 1, :, cols].astype(F32)
        back = PF[1, 0, :, cols] + RB[1, 0, :, cols].astype(F32) + RB[1, 1, :, cols].astype(F32)
        squash = jax.nn.sigmoid(preact)
        ACT[:, cols] = (preact * squash).astype(BF16)
        HG[x, :, cols] = (back * squash * (1.0 + preact * (1.0 - squash))).astype(BF16)

    def add_up(g):
        cols = slice(GROUPS[g][0], sum(GROUPS[g]))
        hq = dot_nt(UQ[:, cols], HG[x, :, cols].astype(F32), HI)
        AU[...] += dot_nn(hq, WIN[0].astype(F32), HI) * grad_scale

    def add_down(g):
        cols = slice(GROUPS[g][0], sum(GROUPS[g]))
        AD[:, cols] += dot_nn(GQ[...], ACT[:, cols].astype(F32), HI) * grad_scale

    def h_copy(g, i):
        cols = pl.ds(*GROUPS[g])
        own = HG.at[x, :, cols]
        src = (own, own, HG.at[xl, top, cols], HG.at[xrr, bot, cols])[i]
        return rcopy(src, src, hs.at[g, i], hr.at[g, i], at_x(xrr if i % 2 == 0 else xl))

    def h_wait(g, i):
        cols = pl.ds(*GROUPS[g])
        x2 = wrap(x + 2, NX)
        ref = (
            HG.at[xl, :, cols], HG.at[xrr, :, cols], HG.at[x2, top, cols], HG.at[x2, bot, cols]
        )[i]
        rcopy(ref, ref, hs.at[g, i], hr.at[g, i], (dp, t)).wait_recv()

    def h_relay(g):
        h_wait(g, 0)
        h_copy(g, 2).start()
        h_wait(g, 1)
        h_copy(g, 3).start()

    ring_arrived(0, 0, 3, 1)
    ring_end(0, 1)
    products(0, 1)
    rs_first(0, 1)
    ring_arrived(1, 0, 3, 1)
    ring_end(1, 1)
    products(1, 1)
    rs_first(1, 1)
    rs_second(0, 1)
    rs_second(1, 1)
    rs_end(0, 0)
    rs_end(1, 0)
    activate(0)
    h_copy(0, 0).start()
    h_copy(0, 1).start()
    add_up(0)
    add_down(0)
    rs_end(0, 1)
    rs_end(1, 1)
    activate(1)

    def along(at, n, visit, here):
        visit(wrap(at + n // 2, n))

        def one(i, carry):
            visit(wrap(at + n // 2 - i, n))
            visit(wrap(at + n // 2 + i, n))
            return carry

        lax.fori_loop(1, n // 2, one, 0)
        here()

    other_x = [wrap(x + d, NX) for d in (2, 1, 3)]

    def dp_others(send):
        def visit(zi):
            for xi in (*other_x, x):
                send(zi * NX + xi)

        def here():
            for xi in other_x:
                send(z * NX + xi)

        along(z, NZ, visit, here)

    def t_others(send):
        def visit(yi):
            send(2 * yi)
            send(2 * yi + 1)

        along(y, NY, visit, lambda: send(2 * y + 1 - c))

    def put28(k, arr):
        for g in range(4):
            for l in range(7):
                P28[k, g * 7 + l] = arr[8 * g : 8 * g + 8, 128 * l : 128 * l + 128]

    def put8(k, arr):
        for g in range(4):
            for l in range(2):
                P8[k, g * 2 + l] = arr[8 * g : 8 * g + 8, 128 * l : 128 * l + 128]

    def get(buf, k, n):
        return jnp.concatenate(
            [jnp.concatenate([buf[k, g * n + l] for l in range(n)], axis=1) for g in range(4)],
            axis=0,
        )

    def send28(k):
        def one(j):
            @pl.when(j < 28)
            def _():
                rcopy(P28.at[k, j], R28.at[k, dp], cs.at[k, 0], cr.at[k, 0], (j, t)).start()

        dp_others(one)

        @pl.when(dp < 28)
        def _():
            R28[k, dp] = P28[k, dp]

    def reduce28(k):
        @pl.when(dp < 28)
        def _():
            drain(R28.at[k, pl.ds(0, 31)], cr.at[k, 0])
            L28[k, dp] = jnp.sum(R28[k], axis=0)

            def one(j):
                rcopy(L28.at[k, dp], L28.at[k, dp], cs.at[k, 1], cr.at[k, 1], (j, t)).start()

            dp_others(one)

    def end28(k):
        @pl.when(dp < 28)
        def _():
            drain(L28.at[k, pl.ds(0, 27)], cr.at[k, 1])

        @pl.when(dp >= 28)
        def _():
            drain(L28.at[k, pl.ds(0, 28)], cr.at[k, 1])

    def send8(k):
        def one(j, carry):
            @pl.when(j != t)
            def _():
                rcopy(P8.at[k, j], R8T.at[k, t], cs.at[k, 2], cr.at[k, 2], (dp, j)).start()

            return carry

        lax.fori_loop(0, 8, one, 0)

        @pl.when(t < 8)
        def _():
            R8T[k, t] = P8[k, t]

    def middle8(k):
        @pl.when(t < 8)
        def _():
            drain(R8T.at[k, pl.ds(0, 15)], cr.at[k, 2])
            R8D[k, dp] = jnp.sum(R8T[k], axis=0)

            def one(j):
                rcopy(R8D.at[k, dp], R8D.at[k, dp], cs.at[k, 3], cr.at[k, 3], (j, t)).start()

            dp_others(one)

    def reduce8(k):
        @pl.when(t < 8)
        def _():
            drain(R8D.at[k, pl.ds(0, 31)], cr.at[k, 3])
            L8[k, t] = jnp.sum(R8D[k], axis=0)

            def one(j):
                rcopy(L8.at[k, t], L8.at[k, t], cs.at[k, 4], cr.at[k, 4], (dp, j)).start()

            t_others(one)

    def end8(k):
        @pl.when(t < 8)
        def _():
            drain(L8.at[k, pl.ds(0, 7)], cr.at[k, 4])

        @pl.when(t >= 8)
        def _():
            drain(L8.at[k, pl.ds(0, 8)], cr.at[k, 4])

    add_up(1)
    put8(0, AU[...])
    send8(0)
    add_down(1)
    put28(0, AD[...])
    send28(0)

    def ig_product(i):
        IGP[i] = dot_nt(HG[i], WU[...].reshape(NZ * 128, WU.shape[2])).astype(BF16)

    h_copy(1, 0).start()
    h_copy(1, 1).start()
    MU[...] += dot_nn(WIN[0].T, HG[x]) * grad_scale
    MD[...] += dot_nn(ACT[...].T, WIN[1]) * grad_scale
    store_u = pltpu.make_async_copy(MU, mu_out, acc_sem.at[0])
    store_d = pltpu.make_async_copy(MD, md_out, acc_sem.at[1])
    store_u.start()
    store_d.start()
    for mat in range(2):
        for g in range(2):
            for step in range(1, 5):
                for way in ring_ways(step, g):
                    ring(mat, way, step, g).wait_send()
            for i in range(6):
                rs_copy(mat, g, i).wait_send()
    for arr in range(2):
        for h in range(2):

            @pl.when(foreign(h))
            def _():
                piece(arr, h).wait_send()

        for off in range(1, NY):
            spread(arr, off).wait_send()
        for off in range(NY):
            to_sibling(arr, wrap(y - off, NY), off).wait_send()

    @pl.when(t == 0)
    def _():
        for arr in range(2):

            def one(j, carry):
                rcopy(WIN.at[arr], WIN.at[arr], ws.at[arr], wr.at[arr], (dp, j)).wait_send()
                return carry

            lax.fori_loop(1, NT, one, 0)

    h_relay(0)
    middle8(0)
    reduce28(0)
    h_relay(1)

    def ig_near(d, carry):
        ig_product(wrap(x + d - 1, NX))
        return carry

    order = (1 - lax.rem(x, 2), lax.rem(x, 2))

    def pair_copy(k):
        i = order[k]
        return rcopy(IGP.at[2 - 2 * c + i], IGX.at[i], ps_s.at[k], ps_r.at[k], sib)

    def pair_sum(k):
        i = order[k]
        rcopy(IGX.at[i], IGX.at[i], ps_s.at[k], ps_r.at[k], sib).wait_recv()
        both = (IGP[2 * c + i].astype(F32) + IGX[i].astype(F32)).astype(BF16)
        for j in range(NY):
            PS[k, j] = both[:, j * 128 : (j + 1) * 128]
        RY[k, y] = PS[k, y]

        def ry_send(j):
            rcopy(PS.at[k, j], RY.at[k, y], ry_s.at[k], ry_r.at[k], (dp, 2 * j + c)).start()

        along(y, NY, ry_send, lambda: None)

    lax.fori_loop(0, 3, ig_near, 0)
    pair_copy(0).start()
    reduce8(0)
    for g in range(2):
        h_wait(g, 2)
        h_wait(g, 3)
    lax.fori_loop(3, 4, ig_near, 0)
    pair_copy(1).start()

    end28(0)
    down_sum = get(L28, 0, 7)
    put8(1, dot_nn(down_sum, MD[...], HI))
    send8(1)
    gram_part = dot_nt(down_sum, down_sum, HI)
    GR[t] = jnp.concatenate([gram_part[8 * g : 8 * g + 8] for g in range(4)], axis=1)

    def gram_send(j):
        rcopy(GR.at[t], GR.at[t], gs.at[0], gr.at[0], (dp, j)).start()

    t_others(gram_send)

    pair_sum(0)
    pair_sum(1)
    end8(0)
    up_sum = get(L8, 0, 2)
    put28(1, dot_nn(up_sum, MU[...], HI))
    send28(1)
    middle8(1)

    def sums_left(k):
        @pl.when(dp < 28)
        def _():
            drain(P28.at[k, pl.ds(0, 27)], cs.at[k, 0])
            drain(R28.at[k, pl.ds(0, 31)], cs.at[k, 1])

        @pl.when(dp >= 28)
        def _():
            drain(P28.at[k, pl.ds(0, 28)], cs.at[k, 0])

        @pl.when(t < 8)
        def _():
            drain(P8.at[k, pl.ds(0, 7)], cs.at[k, 2])
            drain(R8D.at[k, pl.ds(0, 31)], cs.at[k, 3])
            drain(R8T.at[k, pl.ds(0, 15)], cs.at[k, 4])

        @pl.when(t >= 8)
        def _():
            drain(P8.at[k, pl.ds(0, 8)], cs.at[k, 2])

    def put_out(ref, value, dst, i):
        ref[...] = value
        copy = pltpu.make_async_copy(ref, dst, out_sem.at[i])
        copy.start()
        return copy

    results = []
    up_inv = inverse_factor(dot_nt(up_sum, up_sum, HI))
    results.append(put_out(UL, dot_nn(up_inv, up_sum, HI), ul_out, 0))
    store_u.wait()
    store_d.wait()
    sums_left(0)
    for g in range(2):
        for i in range(4):
            h_copy(g, i).wait_send()
    pair_copy(0).wait_send()
    pair_copy(1).wait_send()
    reduce28(1)
    drain(GR.at[pl.ds(0, NT - 1)], gr.at[0])
    packed = jnp.sum(GR[...], axis=0)
    gram = jnp.concatenate([packed[:, 32 * g : 32 * g + 32] for g in range(4)], axis=0)
    reduce8(1)
    down_inv = inverse_factor(gram)
    results.append(put_out(DL, dot_nn(down_inv, down_sum, HI), dl_out, 1))

    for k in range(2):
        drain(RY.at[k, pl.ds(0, NY - 1)], ry_r.at[k])
        FY[order[k]] = jnp.sum(RY[k].astype(F32), axis=0).astype(BF16)

    def last(i, h):
        return rcopy(
            FY.at[i],
            IGO.at[h],
            fs.at[i],
            fr.at[h],
            (z * NX + 2 * c + i, 2 * y + x // 2),
        )

    for h in range(2):
        for i in range(2):

            @pl.when(jnp.logical_and(lax.rem(x, 2) == h, foreign(i)))
            def _():
                last(i, h).start()

        @pl.when(jnp.logical_and(mine, lax.rem(x, 2) == h))
        def _():
            IGO[h] = FY[h]

    end28(1)
    results.append(
        put_out(UR, dot_nn(up_inv, get(L28, 1, 7), HI) * (1.0 / NDP), ur_out, 2)
    )
    end8(1)
    results.append(
        put_out(DR, dot_nn(down_inv, get(L8, 1, 2), HI) * (1.0 / NDP), dr_out, 3)
    )

    for k in range(2):
        drain(PS.at[k, pl.ds(0, NY - 1)], ry_s.at[k])
    sums_left(1)
    drain(GR.at[pl.ds(0, NT - 1)], gs.at[0])
    for h in range(2):

        @pl.when(foreign(h))
        def _():
            rcopy(IGO.at[h], IGO.at[h], fs.at[h], fr.at[h], (dp, t)).wait_recv()

        copy = pltpu.make_async_copy(
            IGO.at[h], ig_out.at[:, pl.ds(h * 128, 128)], out_sem.at[4 + h]
        )
        copy.start()
        results.append(copy)
    for i in range(2):

        @pl.when(foreign(i))
        def _():
            rcopy(FY.at[i], FY.at[i], fs.at[i], fr.at[i], (dp, t)).wait_send()

    for copy in results:
        copy.wait()


def finish(*refs):
    ins, outs, held = refs[:7], refs[7:14], refs[14:21]
    came, left = refs[21], refs[22]
    loads = [pltpu.make_async_copy(ins[i], held[i], came.at[i]) for i in range(7)]
    ends = [outs[i] if i < 5 else outs[i].at[0] for i in range(7)]
    stores = [pltpu.make_async_copy(held[i], ends[i], left.at[i]) for i in range(7)]
    for i in (1, 2, 5, 3, 4, 6, 0):
        loads[i].start()
    for i, low, high in ((5, 1, 2), (6, 3, 4)):
        for k in (low, high, i):
            loads[k].wait()
        held[i][...] -= dot_thirds(held[low][...], held[high][...])
        for k in (i, low, high):
            stores[k].start()
    loads[0].wait()
    stores[0].start()
    for store in stores:
        store.wait()


def shards(tokens, out_grad, up_weight, down_weight, up_accum, down_accum, up_q, down_q):
    rows, feats = tokens.shape
    hid = up_weight.shape[1]
    win = up_accum.shape[1]
    rank = up_q.shape[1]
    quarter = NZ * 128
    hbm = pl.BlockSpec(memory_space=pl.ANY)
    sem = pltpu.SemaphoreType.DMA
    V = pltpu.VMEM
    shape = jax.ShapeDtypeStruct
    outs = pl.pallas_call(
        kernel,
        out_shape=[
            shape((rows, feats), BF16),
            shape((rank, win), F32),
            shape((rank, hid), F32),
            shape((rank, hid), F32),
            shape((rank, win), F32),
            shape((win, hid), F32),
            shape((hid, win), F32),
        ],
        in_specs=[hbm] * 8,
        out_specs=[hbm] * 7,
        scratch_shapes=[
            V((2, rows, feats), BF16),
            V((rows, hid), BF16),
            V((rank, hid), F32),
            V((rank, win), F32),
            V((rank, win), F32),
            V((rank, hid), F32),
            V((rank, rows), F32),
            V((rank, win), F32),
            V((rank, hid), F32),
            V((rank, hid), F32),
            V((rank, win), F32),
            V((2, NX, rows, quarter), BF16),
            V((NZ, 128, hid), BF16),
            V((hid, quarter), BF16),
            V((2, rows, win), BF16),
            V((2, NX, rows, hid), F32),
            V((2, 3, rows, hid), BF16),
            V((2, 2, rows // 2, hid), BF16),
            V((2, 2, rows, hid), BF16),
            V((NX, rows, hid), BF16),
            V((NX, rows, quarter), BF16),
            V((2, rows, quarter), BF16),
            V((2, NY, rows, 128), BF16),
            V((2, NY, rows, 128), BF16),
            V((2, rows, 128), BF16),
            V((2, rows, 128), BF16),
            V((win, hid), F32),
            V((hid, win), F32),
            V((2, 28, 8, 128), F32),
            V((2, NDP, 8, 128), F32),
            V((2, 28, 8, 128), F32),
            V((2, 8, 8, 128), F32),
            V((2, NT, 8, 128), F32),
            V((2, NDP, 8, 128), F32),
            V((2, 8, 8, 128), F32),
            V((NT, 8, 128), F32),
            sem((6,)),
            sem((2,)),
            sem((6,)),
            sem((2, 2, 2, 4)),
            sem((2, 2, 2, 4)),
            sem((2, 2)),
            sem((2, 2)),
            sem((2, NY)),
            sem((2, NY)),
            sem((2, NY)),
            sem((2, NY)),
            sem((2,)),
            sem((2,)),
            sem((2, 2, 6)),
            sem((2, 2, 6)),
            sem((2, 4)),
            sem((2, 4)),
            sem((2,)),
            sem((2,)),
            sem((2,)),
            sem((2,)),
            sem((2,)),
            sem((2,)),
            sem((2, 5)),
            sem((2, 5)),
            sem((1,)),
            sem((1,)),
        ],
        compiler_params=pltpu.CompilerParams(
            collective_id=0, has_side_effects=True, vmem_limit_bytes=63 * 1024 * 1024
        ),
    )(tokens, out_grad, up_weight, down_weight, up_q.T, down_q.T, up_accum, down_accum)
    input_grad, ul, ur, dl, dr, mu, md = outs
    results = pl.pallas_call(
        finish,
        out_shape=[
            shape((rows, feats), BF16),
            shape((rank, win), F32),
            shape((rank, hid), F32),
            shape((rank, hid), F32),
            shape((rank, win), F32),
            shape(up_accum.shape, F32),
            shape(down_accum.shape, F32),
        ],
        in_specs=[hbm] * 7,
        out_specs=[hbm] * 7,
        scratch_shapes=[
            V((rows, feats), BF16),
            V((rank, win), F32),
            V((rank, hid), F32),
            V((rank, hid), F32),
            V((rank, win), F32),
            V((win, hid), F32),
            V((hid, win), F32),
            sem((7,)),
            sem((7,)),
        ],
        compiler_params=pltpu.CompilerParams(vmem_limit_bytes=63 * 1024 * 1024),
    )(input_grad, ul, ur, dl, dr, mu, md)
    input_grad, ul, ur, dl, dr, up_error, down_error = results
    return input_grad, up_error, ul.T, ur.T, down_error, dl.T, dr.T


def solution(mesh):
    return jax.shard_map(
        shards,
        mesh=mesh,
        in_specs=(
            P("dp", "tensor"),
            P("dp", "tensor"),
            P("dp", "tensor"),
            P("tensor", "dp"),
            P("dp", None, "tensor"),
            P("dp", "tensor", None),
            P("tensor", None),
            P(),
        ),
        out_specs=(
            P("dp", "tensor"),
            P("dp", None, "tensor"),
            P(),
            P("tensor", None),
            P("dp", "tensor", None),
            P("tensor", None),
            P(),
        ),
        check_vma=False,
    )
```

```python
import functools
import math

import jax
import jax.numpy as jnp
from jax import lax
from jax.experimental import pallas as pl
from jax.experimental.pallas import tpu as pltpu
from jax.sharding import PartitionSpec as P

MESH = pl.DeviceIdType.MESH
HI = lax.Precision.HIGHEST
NZ, NX, NY = 8, 4, 8
NDP, NT = 32, 16
F32, BF16 = jnp.float32, jnp.bfloat16


def wrap(a, n):
    return lax.rem(a + 4 * n, n)


def thirds(a):
    high = a.astype(BF16)
    rest = a - high.astype(F32)
    middle = rest.astype(BF16)
    return high, middle, (rest - middle.astype(F32)).astype(BF16)


def dot_thirds(left_t, right_t):
    lh, lm, ll = thirds(left_t)
    rh, rm, rl = thirds(right_t)
    left = jnp.concatenate([ll, lm, lh, lm, lh, lh], axis=0)
    right = jnp.concatenate([rh, rm, rl, rh, rm, rh], axis=0)
    return dot_nn(left.astype(F32).T.astype(BF16), right)


def dot_nt(a, b, precision=None):
    return lax.dot_general(
        a, b, (((1,), (1,)), ((), ())), preferred_element_type=F32, precision=precision
    )


def dot_nn(a, b, precision=None):
    return jnp.dot(a, b, preferred_element_type=F32, precision=precision)


def inverse_factor(gram):
    n = gram.shape[0]
    rows = lax.broadcasted_iota(jnp.int32, (n, 128), 0)
    lanes = lax.broadcasted_iota(jnp.int32, (n, 128), 1)
    unit = jnp.where(lanes == rows + n, 1.0, 0.0).astype(F32)
    work = jnp.concatenate([gram, jnp.zeros((n, 128 - n), F32)], axis=1) + unit
    for k in range(n):
        scale = lax.rsqrt(work[k : k + 1, k : k + 1])
        line = work[k : k + 1, :] * scale
        col = work[:, k : k + 1] * scale
        work = jnp.where(rows > k, work - col * line, jnp.where(rows == k, line, work))
    return work[:, n : 2 * n]


GROUPS = ((0, 512), (512, 384))


def kernel(
    tok_in, og_in, wu_in, wd_in, uq_in, dq_in, uacc, dacc,
    ig_out, ul_out, ur_out, dl_out, dr_out, mu_out, md_out,
    TO, ACT, UQ, DQ, AU, AD, GQ, UL, UR, DL, DR,
    A, WU, WD, WIN, PF, SB, FB, RB, HG, IGP, IGX, PS, RY, FY, IGO, MU, MD,
    P28, R28, L28, P8, R8T, R8D, L8, GR,
    in_sem, acc_sem, out_sem, ring_s, ring_r, xs, xr, ys, yr, ds, dr, ws, wr,
    rs_s, rs_r, hs, hr, ps_s, ps_r, ry_s, ry_r, fs, fr, cs, cr, gs, gr,
):
    dp, t = lax.axis_index("dp"), lax.axis_index("tensor")
    z, x = dp // NX, lax.rem(dp, NX)
    y, c = t // 2, lax.rem(t, 2)
    mine = x // 2 == c
    xl, xrr = wrap(x - 1, NX), wrap(x + 1, NX)
    sib = (dp, t + 1 - 2 * c)
    tok, og = TO.at[0], TO.at[1]
    tokens = TO.shape[1]
    grad_scale = 1.0 / math.sqrt(tokens)

    def lanes_of(i):
        return pl.ds(pl.multiple_of(i * 128, 128), 128)

    def rcopy(src, dst, s, r, dev):
        return pltpu.make_async_remote_copy(
            src_ref=src, dst_ref=dst, send_sem=s, recv_sem=r, device_id=dev, device_id_type=MESH
        )

    def drain(ref, sem):
        pltpu.make_async_copy(ref, ref, sem).wait()

    def at_x(xi):
        return (z * NX + xi, t)

    loads = [
        pltpu.make_async_copy(src, dst, in_sem.at[i])
        for i, (src, dst) in enumerate(
            (
                (wu_in, WU.at[z]),
                (wd_in, WD.at[:, lanes_of(z)]),
                (tok_in, tok),
                (og_in, og),
                (uq_in, UQ),
                (dq_in, DQ),
            )
        )
    ]
    load_u = pltpu.make_async_copy(uacc.at[0], MU, acc_sem.at[0])
    load_d = pltpu.make_async_copy(dacc.at[0], MD, acc_sem.at[1])
    for load in loads:
        load.start()
    load_u.start()
    load_d.start()

    barrier = pltpu.get_barrier_semaphore()

    def greet_dp(j, carry):
        @pl.when(j != dp)
        def _():
            pl.semaphore_signal(barrier, inc=1, device_id=(j, t), device_id_type=MESH)

        return carry

    def greet_t(j, carry):
        @pl.when(j != t)
        def _():
            pl.semaphore_signal(barrier, inc=1, device_id=(dp, j), device_id_type=MESH)

        return carry

    lax.fori_loop(0, NDP, greet_dp, 0)
    lax.fori_loop(0, NT, greet_t, 0)

    @pl.when(jnp.logical_not(mine))
    def _():
        for h in range(2):
            pl.semaphore_signal(
                barrier,
                inc=1,
                device_id=(z * NX + 2 * c + h, 2 * y + x // 2),
                device_id_type=MESH,
            )

    for load in loads[:4]:
        load.wait()
    for h in range(2):

        @pl.when(jnp.logical_and(mine, lax.rem(x, 2) == h))
        def _():
            for arr in range(2):
                A[arr, x, :, lanes_of(y)] = TO[arr, :, h * 128 : (h + 1) * 128]

    @pl.when(t == 0)
    def _():
        WIN[...] = TO[...]

    pl.semaphore_wait(barrier, NDP + NT - 2 + 2 * jnp.where(mine, 0, 1).astype(jnp.int32))

    def slot(mat, zi, g):
        hidden_range = pl.ds(*GROUPS[g])
        if mat == 0:
            return WU.at[zi, :, hidden_range]
        return WD.at[hidden_range, lanes_of(zi)]

    def ring(mat, way, step, g):
        if way == 0:
            zi, to = wrap(z - step + 1, NZ), wrap(z + 1, NZ)
        else:
            zi, to = wrap(z + step - 1, NZ), wrap(z - 1, NZ)
        i = (mat, way, g, step - 1)
        ref = slot(mat, zi, g)
        return rcopy(ref, ref, ring_s.at[i], ring_r.at[i], (to * NX + x, t))

    def ring_ways(step, g):
        return (0, 1) if step < 4 else (g,)

    def ring_send(mat, step, g):
        for way in ring_ways(step, g):
            ring(mat, way, step, g).start()

    def ring_arrived(mat, way, step, g):
        zi = wrap(z - step, NZ) if way == 0 else wrap(z + step, NZ)
        ref = slot(mat, zi, g)
        i = (mat, way, g, step - 1)
        rcopy(ref, ref, ring_s.at[i], ring_r.at[i], (dp, t)).wait_recv()

    def ring_pass(mat, step, g):
        for way in ring_ways(step - 1, g):
            ring_arrived(mat, way, step - 1, g)
            if way in ring_ways(step, g):
                ring(mat, way, step, g).start()

    def ring_hop(mat, way, step, g):
        ring_arrived(mat, way, step - 1, g)
        ring(mat, way, step, g).start()

    def ring_end(mat, g):
        for way in ring_ways(4, g):
            ring_arrived(mat, way, 4, g)

    ring_send(0, 1, 0)
    ring_send(1, 1, 0)

    def piece(arr, h):
        xd = 2 * c + h
        src = TO.at[arr, :, pl.ds(h * 128, 128)]
        return rcopy(
            src,
            A.at[arr, x, :, lanes_of(y)],
            xs.at[arr, h],
            xr.at[arr, lax.rem(x, 2)],
            (z * NX + xd, 2 * y + x // 2),
        )

    def foreign(h):
        return jnp.logical_not(jnp.logical_and(mine, lax.rem(x, 2) == h))

    for arr in range(2):
        for h in range(2):

            @pl.when(foreign(h))
            def _():
                piece(arr, h).start()

    def pair(arr, yi):
        return A.at[arr, pl.ds(2 * c, 2), :, lanes_of(yi)]

    def spread(arr, off):
        yd = wrap(y + off, NY)
        return rcopy(pair(arr, y), pair(arr, y), ys.at[arr, off], yr.at[arr, off], (dp, 2 * yd + c))

    def to_sibling(arr, yi, off):
        return rcopy(pair(arr, yi), pair(arr, yi), ds.at[arr, off], dr.at[arr, off], sib)

    for arr in range(2):
        for h in range(2):

            @pl.when(foreign(h))
            def _():
                ref = A.at[arr, 2 * c + h, :, lanes_of(y)]
                rcopy(ref, ref, xs.at[arr, h], xr.at[arr, h], (dp, t)).wait_recv()

        for off in (4, 3, 5, 2, 6, 1, 7):
            spread(arr, off).start()
        to_sibling(arr, y, 0).start()

    @pl.when(t == 0)
    def _():
        def one(j, carry):
            rcopy(tok, WIN.at[0], ws.at[0], wr.at[0], (dp, j)).start()
            rcopy(og, WIN.at[1], ws.at[1], wr.at[1], (dp, j)).start()
            return carry

        lax.fori_loop(1, NT, one, 0)

    def y_arrivals(arr):
        for off in (1, 7, 2, 6, 3, 5, 4):
            yi = wrap(y - off, NY)
            ref = pair(arr, yi)
            rcopy(ref, ref, ys.at[arr, off], yr.at[arr, off], (dp, t)).wait_recv()
            to_sibling(arr, yi, off).start()

    def sibling_arrivals(arr):
        for off in range(NY):
            yi = wrap(y - off, NY)
            ref = A.at[arr, pl.ds(2 - 2 * c, 2), :, lanes_of(yi)]
            rcopy(ref, ref, ds.at[arr, off], dr.at[arr, off], (dp, t)).wait_recv()

    def products(mat, g):
        lo, size = GROUPS[g]
        cols = slice(lo, lo + size)

        def one(d, carry):
            xi = wrap(x + d, NX)
            if mat == 0:
                PF[0, d, :, cols] = dot_nn(A[0, xi], WU[:, :, cols].reshape(NZ * 128, size))
            else:
                PF[1, d, :, cols] = dot_nt(A[1, xi], WD[cols, :])
            return carry

        lax.fori_loop(0, NX, one, 0)

    half_rows = tokens // 2
    top, bot = pl.ds(0, half_rows), pl.ds(half_rows, half_rows)

    def rs_copy(mat, g, i):
        cols = pl.ds(*GROUPS[g])
        src = (SB.at[mat, 1, top, cols], SB.at[mat, 1, bot, cols], SB.at[mat, 0, bot, cols],
               SB.at[mat, 2, top, cols], SB.at[mat, 0, top, cols], SB.at[mat, 2, bot, cols])[i]
        dst = (FB.at[mat, 0, :, cols], FB.at[mat, 1, :, cols], RB.at[mat, 0, bot, cols],
               RB.at[mat, 1, top, cols], RB.at[mat, 0, top, cols], RB.at[mat, 1, bot, cols])[i]
        to = at_x(xrr if i % 2 == 0 else xl)
        return rcopy(src, dst, rs_s.at[mat, g, i], rs_r.at[mat, g, i], to)

    def rs_first(mat, g):
        cols = slice(GROUPS[g][0], sum(GROUPS[g]))
        SB[mat, 1, :, cols] = PF[mat, 2, :, cols].astype(BF16)
        rs_copy(mat, g, 0).start()
        rs_copy(mat, g, 1).start()
        SB[mat, 0, half_rows:, cols] = PF[mat, 1, half_rows:, cols].astype(BF16)
        rs_copy(mat, g, 2).start()
        SB[mat, 2, :half_rows, cols] = PF[mat, 3, :half_rows, cols].astype(BF16)
        rs_copy(mat, g, 3).start()

    def rs_second(mat, g):
        cols = slice(GROUPS[g][0], sum(GROUPS[g]))
        rs_copy(mat, g, 0).wait_recv()
        SB[mat, 0, :half_rows, cols] = (
            PF[mat, 1, :half_rows, cols] + FB[mat, 0, :, cols].astype(F32)
        ).astype(BF16)
        rs_copy(mat, g, 4).start()
        rs_copy(mat, g, 1).wait_recv()
        SB[mat, 2, half_rows:, cols] = (
            PF[mat, 3, half_rows:, cols] + FB[mat, 1, :, cols].astype(F32)
        ).astype(BF16)
        rs_copy(mat, g, 5).start()

    def rs_end(mat, g):
        for i in range(2, 6):
            rs_copy(mat, g, i).wait_recv()

    ring_pass(0, 2, 0)
    ring_pass(1, 2, 0)
    loads[4].wait()
    load_u.wait()
    AU[...] = dot_nt(UQ[...], MU[...], HI)
    ring_pass(0, 3, 0)
    ring_pass(1, 3, 0)
    for mat in range(2):
        ring(mat, 1, 1, 1).start()
    loads[5].wait()
    load_d.wait()
    AD[...] = dot_nt(DQ[...], MD[...], HI)
    for mat in range(2):
        ring_hop(mat, 0, 4, 0)
    for mat in range(2):
        ring_arrived(mat, 1, 3, 0)
    for mat in range(2):
        ring(mat, 0, 1, 1).start()
    y_arrivals(0)
    for mat in range(2):
        ring_hop(mat, 1, 2, 1)
    ring_end(0, 0)
    sibling_arrivals(0)
    products(0, 0)
    rs_first(0, 0)
    ring_hop(0, 1, 3, 1)
    ring_end(1, 0)
    ring_hop(1, 1, 3, 1)
    for mat in range(2):
        ring_hop(mat, 0, 2, 1)
    y_arrivals(1)
    sibling_arrivals(1)
    products(1, 0)
    rs_first(1, 0)
    rs_second(0, 0)
    for mat in range(2):
        ring_hop(mat, 1, 4, 1)
    for mat in range(2):
        ring_hop(mat, 0, 3, 1)

    @pl.when(t != 0)
    def _():
        for arr in range(2):
            rcopy(WIN.at[arr], WIN.at[arr], ws.at[arr], wr.at[arr], (dp, t)).wait_recv()

    GQ[...] = dot_nt(DQ[...], WIN[1].astype(F32), HI)
    rs_second(1, 0)

    def activate(g):
        cols = slice(GROUPS[g][0], sum(GROUPS[g]))
        preact = PF[0, 0, :, cols] + RB[0, 0, :, cols].astype(F32) + RB[0, 1, :, cols].astype(F32)
        back = PF[1, 0, :, cols] + RB[1, 0, :, cols].astype(F32) + RB[1, 1, :, cols].astype(F32)
        squash = jax.nn.sigmoid(preact)
        ACT[:, cols] = (preact * squash).astype(BF16)
        HG[x, :, cols] = (back * squash * (1.0 + preact * (1.0 - squash))).astype(BF16)

    def add_up(g):
        cols = slice(GROUPS[g][0], sum(GROUPS[g]))
        hq = dot_nt(UQ[:, cols], HG[x, :, cols].astype(F32), HI)
        AU[...] += dot_nn(hq, WIN[0].astype(F32), HI) * grad_scale

    def add_down(g):
        cols = slice(GROUPS[g][0], sum(GROUPS[g]))
        AD[:, cols] += dot_nn(GQ[...], ACT[:, cols].astype(F32), HI) * grad_scale

    def h_copy(g, i):
        cols = pl.ds(*GROUPS[g])
        own = HG.at[x, :, cols]
        src = (own, own, HG.at[xl, top, cols], HG.at[xrr, bot, cols])[i]
        return rcopy(src, src, hs.at[g, i], hr.at[g, i], at_x(xrr if i % 2 == 0 else xl))

    def h_wait(g, i):
        cols = pl.ds(*GROUPS[g])
        x2 = wrap(x + 2, NX)
        ref = (
            HG.at[xl, :, cols], HG.at[xrr, :, cols], HG.at[x2, top, cols], HG.at[x2, bot, cols]
        )[i]
        rcopy(ref, ref, hs.at[g, i], hr.at[g, i], (dp, t)).wait_recv()

    def h_relay(g):
        h_wait(g, 0)
        h_copy(g, 2).start()
        h_wait(g, 1)
        h_copy(g, 3).start()

    ring_arrived(0, 0, 3, 1)
    ring_end(0, 1)
    products(0, 1)
    rs_first(0, 1)
    ring_arrived(1, 0, 3, 1)
    ring_end(1, 1)
    products(1, 1)
    rs_first(1, 1)
    rs_second(0, 1)
    rs_second(1, 1)
    rs_end(0, 0)
    rs_end(1, 0)
    activate(0)
    h_copy(0, 0).start()
    h_copy(0, 1).start()
    add_up(0)
    add_down(0)
    rs_end(0, 1)
    rs_end(1, 1)
    activate(1)

    def along(at, n, visit, here):
        visit(wrap(at + n // 2, n))

        def one(i, carry):
            visit(wrap(at + n // 2 - i, n))
            visit(wrap(at + n // 2 + i, n))
            return carry

        lax.fori_loop(1, n // 2, one, 0)
        here()

    other_x = [wrap(x + d, NX) for d in (2, 1, 3)]

    def dp_others(send):
        def visit(zi):
            for xi in (*other_x, x):
                send(zi * NX + xi)

        def here():
            for xi in other_x:
                send(z * NX + xi)

        along(z, NZ, visit, here)

    def t_others(send):
        def visit(yi):
            send(2 * yi)
            send(2 * yi + 1)

        along(y, NY, visit, lambda: send(2 * y + 1 - c))

    def put28(k, arr):
        for g in range(4):
            for l in range(7):
                P28[k, g * 7 + l] = arr[8 * g : 8 * g + 8, 128 * l : 128 * l + 128]

    def put8(k, arr):
        for g in range(4):
            for l in range(2):
                P8[k, g * 2 + l] = arr[8 * g : 8 * g + 8, 128 * l : 128 * l + 128]

    def get(buf, k, n):
        return jnp.concatenate(
            [jnp.concatenate([buf[k, g * n + l] for l in range(n)], axis=1) for g in range(4)],
            axis=0,
        )

    def send28(k):
        def one(j):
            @pl.when(j < 28)
            def _():
                rcopy(P28.at[k, j], R28.at[k, dp], cs.at[k, 0], cr.at[k, 0], (j, t)).start()

        dp_others(one)

        @pl.when(dp < 28)
        def _():
            R28[k, dp] = P28[k, dp]

    def reduce28(k):
        @pl.when(dp < 28)
        def _():
            drain(R28.at[k, pl.ds(0, 31)], cr.at[k, 0])
            L28[k, dp] = jnp.sum(R28[k], axis=0)

            def one(j):
                rcopy(L28.at[k, dp], L28.at[k, dp], cs.at[k, 1], cr.at[k, 1], (j, t)).start()

            dp_others(one)

    def end28(k):
        @pl.when(dp < 28)
        def _():
            drain(L28.at[k, pl.ds(0, 27)], cr.at[k, 1])

        @pl.when(dp >= 28)
        def _():
            drain(L28.at[k, pl.ds(0, 28)], cr.at[k, 1])

    def send8(k):
        def one(j, carry):
            @pl.when(j != t)
            def _():
                rcopy(P8.at[k, j], R8T.at[k, t], cs.at[k, 2], cr.at[k, 2], (dp, j)).start()

            return carry

        lax.fori_loop(0, 8, one, 0)

        @pl.when(t < 8)
        def _():
            R8T[k, t] = P8[k, t]

    def middle8(k):
        @pl.when(t < 8)
        def _():
            drain(R8T.at[k, pl.ds(0, 15)], cr.at[k, 2])
            R8D[k, dp] = jnp.sum(R8T[k], axis=0)

            def one(j):
                rcopy(R8D.at[k, dp], R8D.at[k, dp], cs.at[k, 3], cr.at[k, 3], (j, t)).start()

            dp_others(one)

    def reduce8(k):
        @pl.when(t < 8)
        def _():
            drain(R8D.at[k, pl.ds(0, 31)], cr.at[k, 3])
            L8[k, t] = jnp.sum(R8D[k], axis=0)

            def one(j):
                rcopy(L8.at[k, t], L8.at[k, t], cs.at[k, 4], cr.at[k, 4], (dp, j)).start()

            t_others(one)

    def end8(k):
        @pl.when(t < 8)
        def _():
            drain(L8.at[k, pl.ds(0, 7)], cr.at[k, 4])

        @pl.when(t >= 8)
        def _():
            drain(L8.at[k, pl.ds(0, 8)], cr.at[k, 4])

    add_down(1)
    put28(0, AD[...])
    send28(0)
    add_up(1)
    put8(0, AU[...])
    send8(0)

    def ig_product(i):
        IGP[i] = dot_nt(HG[i], WU[...].reshape(NZ * 128, WU.shape[2])).astype(BF16)

    h_copy(1, 0).start()
    h_copy(1, 1).start()
    MU[...] += dot_nn(WIN[0].T, HG[x]) * grad_scale
    MD[...] += dot_nn(ACT[...].T, WIN[1]) * grad_scale
    store_u = pltpu.make_async_copy(MU, mu_out, acc_sem.at[0])
    store_d = pltpu.make_async_copy(MD, md_out, acc_sem.at[1])
    store_u.start()
    store_d.start()
    for mat in range(2):
        for g in range(2):
            for step in range(1, 5):
                for way in ring_ways(step, g):
                    ring(mat, way, step, g).wait_send()
            for i in range(6):
                rs_copy(mat, g, i).wait_send()
    for arr in range(2):
        for h in range(2):

            @pl.when(foreign(h))
            def _():
                piece(arr, h).wait_send()

        for off in range(1, NY):
            spread(arr, off).wait_send()
        for off in range(NY):
            to_sibling(arr, wrap(y - off, NY), off).wait_send()

    @pl.when(t == 0)
    def _():
        for arr in range(2):

            def one(j, carry):
                rcopy(WIN.at[arr], WIN.at[arr], ws.at[arr], wr.at[arr], (dp, j)).wait_send()
                return carry

            lax.fori_loop(1, NT, one, 0)

    h_relay(0)
    middle8(0)
    reduce28(0)
    h_relay(1)

    def ig_near(d, carry):
        ig_product(wrap(x + d - 1, NX))
        return carry

    order = (1 - lax.rem(x, 2), lax.rem(x, 2))

    def pair_copy(k):
        i = order[k]
        return rcopy(IGP.at[2 - 2 * c + i], IGX.at[i], ps_s.at[k], ps_r.at[k], sib)

    def pair_sum(k):
        i = order[k]
        rcopy(IGX.at[i], IGX.at[i], ps_s.at[k], ps_r.at[k], sib).wait_recv()
        both = (IGP[2 * c + i].astype(F32) + IGX[i].astype(F32)).astype(BF16)
        for j in range(NY):
            PS[k, j] = both[:, j * 128 : (j + 1) * 128]
        RY[k, y] = PS[k, y]

        def ry_send(j):
            rcopy(PS.at[k, j], RY.at[k, y], ry_s.at[k], ry_r.at[k], (dp, 2 * j + c)).start()

        along(y, NY, ry_send, lambda: None)

    lax.fori_loop(0, 3, ig_near, 0)
    pair_copy(0).start()
    reduce8(0)
    for g in range(2):
        h_wait(g, 2)
        h_wait(g, 3)
    lax.fori_loop(3, 4, ig_near, 0)
    pair_copy(1).start()

    end28(0)
    down_sum = get(L28, 0, 7)
    put8(1, dot_nn(down_sum, MD[...], HI))
    send8(1)
    gram_part = dot_nt(down_sum, down_sum, HI)
    GR[t] = jnp.concatenate([gram_part[8 * g : 8 * g + 8] for g in range(4)], axis=1)

    def gram_send(j):
        rcopy(GR.at[t], GR.at[t], gs.at[0], gr.at[0], (dp, j)).start()

    t_others(gram_send)

    pair_sum(0)
    pair_sum(1)
    end8(0)
    up_sum = get(L8, 0, 2)
    put28(1, dot_nn(up_sum, MU[...], HI))
    send28(1)
    middle8(1)

    def sums_left(k):
        @pl.when(dp < 28)
        def _():
            drain(P28.at[k, pl.ds(0, 27)], cs.at[k, 0])
            drain(R28.at[k, pl.ds(0, 31)], cs.at[k, 1])

        @pl.when(dp >= 28)
        def _():
            drain(P28.at[k, pl.ds(0, 28)], cs.at[k, 0])

        @pl.when(t < 8)
        def _():
            drain(P8.at[k, pl.ds(0, 7)], cs.at[k, 2])
            drain(R8D.at[k, pl.ds(0, 31)], cs.at[k, 3])
            drain(R8T.at[k, pl.ds(0, 15)], cs.at[k, 4])

        @pl.when(t >= 8)
        def _():
            drain(P8.at[k, pl.ds(0, 8)], cs.at[k, 2])

    def put_out(ref, value, dst, i):
        ref[...] = value
        copy = pltpu.make_async_copy(ref, dst, out_sem.at[i])
        copy.start()
        return copy

    results = []
    up_inv = inverse_factor(dot_nt(up_sum, up_sum, HI))
    results.append(put_out(UL, dot_nn(up_inv, up_sum, HI), ul_out, 0))
    store_u.wait()
    store_d.wait()
    sums_left(0)
    for g in range(2):
        for i in range(4):
            h_copy(g, i).wait_send()
    pair_copy(0).wait_send()
    pair_copy(1).wait_send()
    reduce28(1)
    drain(GR.at[pl.ds(0, NT - 1)], gr.at[0])
    packed = jnp.sum(GR[...], axis=0)
    gram = jnp.concatenate([packed[:, 32 * g : 32 * g + 32] for g in range(4)], axis=0)
    reduce8(1)
    down_inv = inverse_factor(gram)
    results.append(put_out(DL, dot_nn(down_inv, down_sum, HI), dl_out, 1))

    for k in range(2):
        drain(RY.at[k, pl.ds(0, NY - 1)], ry_r.at[k])
        FY[order[k]] = jnp.sum(RY[k].astype(F32), axis=0).astype(BF16)

    def last(i, h):
        return rcopy(
            FY.at[i],
            IGO.at[h],
            fs.at[i],
            fr.at[h],
            (z * NX + 2 * c + i, 2 * y + x // 2),
        )

    for h in range(2):
        for i in range(2):

            @pl.when(jnp.logical_and(lax.rem(x, 2) == h, foreign(i)))
            def _():
                last(i, h).start()

        @pl.when(jnp.logical_and(mine, lax.rem(x, 2) == h))
        def _():
            IGO[h] = FY[h]

    end28(1)
    results.append(
        put_out(UR, dot_nn(up_inv, get(L28, 1, 7), HI) * (1.0 / NDP), ur_out, 2)
    )
    end8(1)
    results.append(
        put_out(DR, dot_nn(down_inv, get(L8, 1, 2), HI) * (1.0 / NDP), dr_out, 3)
    )

    for k in range(2):
        drain(PS.at[k, pl.ds(0, NY - 1)], ry_s.at[k])
    sums_left(1)
    drain(GR.at[pl.ds(0, NT - 1)], gs.at[0])
    for h in range(2):

        @pl.when(foreign(h))
        def _():
            rcopy(IGO.at[h], IGO.at[h], fs.at[h], fr.at[h], (dp, t)).wait_recv()

        copy = pltpu.make_async_copy(
            IGO.at[h], ig_out.at[:, pl.ds(h * 128, 128)], out_sem.at[4 + h]
        )
        copy.start()
        results.append(copy)
    for i in range(2):

        @pl.when(foreign(i))
        def _():
            rcopy(FY.at[i], FY.at[i], fs.at[i], fr.at[i], (dp, t)).wait_send()

    for copy in results:
        copy.wait()


def finish(*refs):
    ins, outs, held = refs[:7], refs[7:14], refs[14:21]
    came, left = refs[21], refs[22]
    loads = [pltpu.make_async_copy(ins[i], held[i], came.at[i]) for i in range(7)]
    ends = [outs[i] if i < 5 else outs[i].at[0] for i in range(7)]
    stores = [pltpu.make_async_copy(held[i], ends[i], left.at[i]) for i in range(7)]
    for i in (1, 2, 5, 3, 4, 6, 0):
        loads[i].start()
    for i, low, high in ((5, 1, 2), (6, 3, 4)):
        for k in (low, high, i):
            loads[k].wait()
        held[i][...] -= dot_thirds(held[low][...], held[high][...])
        for k in (i, low, high):
            stores[k].start()
    loads[0].wait()
    stores[0].start()
    for store in stores:
        store.wait()


def shards(tokens, out_grad, up_weight, down_weight, up_accum, down_accum, up_q, down_q):
    rows, feats = tokens.shape
    hid = up_weight.shape[1]
    win = up_accum.shape[1]
    rank = up_q.shape[1]
    quarter = NZ * 128
    hbm = pl.BlockSpec(memory_space=pl.ANY)
    sem = pltpu.SemaphoreType.DMA
    V = pltpu.VMEM
    shape = jax.ShapeDtypeStruct
    outs = pl.pallas_call(
        kernel,
        out_shape=[
            shape((rows, feats), BF16),
            shape((rank, win), F32),
            shape((rank, hid), F32),
            shape((rank, hid), F32),
            shape((rank, win), F32),
            shape((win, hid), F32),
            shape((hid, win), F32),
        ],
        in_specs=[hbm] * 8,
        out_specs=[hbm] * 7,
        scratch_shapes=[
            V((2, rows, feats), BF16),
            V((rows, hid), BF16),
            V((rank, hid), F32),
            V((rank, win), F32),
            V((rank, win), F32),
            V((rank, hid), F32),
            V((rank, rows), F32),
            V((rank, win), F32),
            V((rank, hid), F32),
            V((rank, hid), F32),
            V((rank, win), F32),
            V((2, NX, rows, quarter), BF16),
            V((NZ, 128, hid), BF16),
            V((hid, quarter), BF16),
            V((2, rows, win), BF16),
            V((2, NX, rows, hid), F32),
            V((2, 3, rows, hid), BF16),
            V((2, 2, rows // 2, hid), BF16),
            V((2, 2, rows, hid), BF16),
            V((NX, rows, hid), BF16),
            V((NX, rows, quarter), BF16),
            V((2, rows, quarter), BF16),
            V((2, NY, rows, 128), BF16),
            V((2, NY, rows, 128), BF16),
            V((2, rows, 128), BF16),
            V((2, rows, 128), BF16),
            V((win, hid), F32),
            V((hid, win), F32),
            V((2, 28, 8, 128), F32),
            V((2, NDP, 8, 128), F32),
            V((2, 28, 8, 128), F32),
            V((2, 8, 8, 128), F32),
            V((2, NT, 8, 128), F32),
            V((2, NDP, 8, 128), F32),
            V((2, 8, 8, 128), F32),
            V((NT, 8, 128), F32),
            sem((6,)),
            sem((2,)),
            sem((6,)),
            sem((2, 2, 2, 4)),
            sem((2, 2, 2, 4)),
            sem((2, 2)),
            sem((2, 2)),
            sem((2, NY)),
            sem((2, NY)),
            sem((2, NY)),
            sem((2, NY)),
            sem((2,)),
            sem((2,)),
            sem((2, 2, 6)),
            sem((2, 2, 6)),
            sem((2, 4)),
            sem((2, 4)),
            sem((2,)),
            sem((2,)),
            sem((2,)),
            sem((2,)),
            sem((2,)),
            sem((2,)),
            sem((2, 5)),
            sem((2, 5)),
            sem((1,)),
            sem((1,)),
        ],
        compiler_params=pltpu.CompilerParams(
            collective_id=0, has_side_effects=True, vmem_limit_bytes=63 * 1024 * 1024
        ),
    )(tokens, out_grad, up_weight, down_weight, up_q.T, down_q.T, up_accum, down_accum)
    input_grad, ul, ur, dl, dr, mu, md = outs
    results = pl.pallas_call(
        finish,
        out_shape=[
            shape((rows, feats), BF16),
            shape((rank, win), F32),
            shape((rank, hid), F32),
            shape((rank, hid), F32),
            shape((rank, win), F32),
            shape(up_accum.shape, F32),
            shape(down_accum.shape, F32),
        ],
        in_specs=[hbm] * 7,
        out_specs=[hbm] * 7,
        scratch_shapes=[
            V((rows, feats), BF16),
            V((rank, win), F32),
            V((rank, hid), F32),
            V((rank, hid), F32),
            V((rank, win), F32),
            V((win, hid), F32),
            V((hid, win), F32),
            sem((7,)),
            sem((7,)),
        ],
        compiler_params=pltpu.CompilerParams(vmem_limit_bytes=63 * 1024 * 1024),
    )(input_grad, ul, ur, dl, dr, mu, md)
    input_grad, ul, ur, dl, dr, up_error, down_error = results
    return input_grad, up_error, ul.T, ur.T, down_error, dl.T, dr.T


def solution(mesh):
    return jax.shard_map(
        shards,
        mesh=mesh,
        in_specs=(
            P("dp", "tensor"),
            P("dp", "tensor"),
            P("dp", "tensor"),
            P("tensor", "dp"),
            P("dp", None, "tensor"),
            P("dp", "tensor", None),
            P("tensor", None),
            P(),
        ),
        out_specs=(
            P("dp", "tensor"),
            P("dp", None, "tensor"),
            P(),
            P("tensor", None),
            P("dp", "tensor", None),
            P("tensor", None),
            P(),
        ),
        check_vma=False,
    )
```
